32 devices in a mesh: dp: 8 (over z, x), mp: 4 (over y, core).
Axes of the slice: x: 2, y: 2, z: 4, core: 2. Of those that a mesh axis runs over, the one named last changes fastest.
Arguments:
- grads: bfloat16 [8, 4, 4096, 256], P('dp', 'mp'), may hold values from -6 to 6
- master: float32 [4, 4096, 256], P('mp', 'dp'), may hold values from -6 to 6
- m_codes: bfloat16 [4, 4096, 256], P('mp', 'dp'), may hold values from -1 to 1
- m_scale: float32 [4, 4096], P('mp', 'dp'), may hold values from 0.005 to 0.05
- v_codes: bfloat16 [4, 4096, 256], P('mp', 'dp'), may hold values from 0.049804688 to 1
- v_scale: float32 [4, 4096], P('mp', 'dp'), may hold values from 0.001 to 0.01
Outputs:
- master_out: float32 [4, 4096, 256], P('mp', 'dp')
- m_codes_out: bfloat16 [4, 4096, 256], P('mp', 'dp')
- m_scale_out: float32 [4, 4096], P('mp', 'dp')
- v_codes_out: bfloat16 [4, 4096, 256], P('mp', 'dp')
- v_scale_out: float32 [4, 4096], P('mp', 'dp')
- weights: bfloat16 [4, 4096, 256], P('mp')
The draws below stay inside these ranges and needn't reach their ends.
All inputs are finite; a program needn't handle non-finite values. Where the reference program divides by a largest or mean magnitude, that divisor is 1e-20 or more.
Results may differ from the reference program's by a relative error of at most 0.024.
Values may be sent and summed in bfloat16 or wider, within the bound.
A program may use at most 128 MiB of HBM per device.

```python
import math
import jax
import jax.numpy as jnp
from jax import lax

BLOCK = 256
OWNB = 512
STEP = 8
MPB = 4096
LEVELS = 3
N_DP = 8
N_MP = 4


def raised(array, rng, source, target, shards_of, factor):
    def block_of(dim):
        return (jnp.arange(array.shape[dim]) // (array.shape[dim] // shards_of)).reshape((-1,) + (1,) * (array.ndim - 1 - dim))

    one_side = jax.random.permutation(rng, shards_of)[block_of(target)]
    other_side = (block_of(target) + shards_of // 2) % shards_of
    return jnp.where((block_of(source) == one_side) | (block_of(source) == other_side), factor * array, array)


def level_of(stream_key, dims, cuts, smallest, largest):
    factor_of = 1.0
    for position, shards_of in cuts:
        heights = jax.random.uniform(jax.random.fold_in(jax.random.fold_in(stream_key, 6), position), (shards_of,), jnp.float32, smallest / len(cuts), largest / len(cuts))
        factor_of = factor_of * jnp.repeat(jnp.exp(heights), dims[position] // shards_of).reshape((-1,) + (1,) * (len(dims) - 1 - position))
    return factor_of


def gaussian(rng, shape, scale, bound, shards=(), kind=jnp.bfloat16):
    result = jax.random.normal(rng, shape, jnp.float32) * scale
    if len(shards) > 0:
        result = level_of(rng, shape, shards, -0.22, 0.18) * result
    return jnp.clip(result, min=-bound, max=bound).astype(kind)


def gaussian_with(key, shape, width, most, shards, heavy, kind=jnp.bfloat16):
    array = width * jax.random.normal(key, shape, jnp.float32)
    if shards:
        array = array * level_of(key, shape, shards, -0.22, 0.18)
    return jnp.clip(raised(array, jax.random.fold_in(key, 3), *heavy), -most, most).astype(kind)


def setup_inputs(seed: int = 0) -> dict:
    arg_keys = jax.random.split(jax.random.key(seed), 7)
    grads = gaussian_with(arg_keys[0], (N_DP, N_MP, MPB, BLOCK), 1.0, 6.0, ((0, 8), (1, 4)), (0, 2, 8, 2.0))
    master = gaussian(arg_keys[1], (N_MP, MPB, BLOCK), 1.0, 6.0, ((0, 4), (1, 8)), jnp.float32)
    m_codes = jnp.clip(jax.random.uniform(arg_keys[2], (N_MP, MPB, BLOCK), jnp.float32, -1.0, 1.0) * level_of(arg_keys[2], (N_MP, MPB, BLOCK), ((0, 4), (1, 8)), -0.4, 0.0), -1.0, 1.0).astype(jnp.bfloat16)
    m_scale = jnp.clip(jnp.exp(math.log(0.05) - 2.3025851 * jax.random.uniform(arg_keys[3], (N_MP, MPB), jnp.float32) ** level_of(arg_keys[3], (N_MP, MPB), ((0, 4), (1, 8)), -0.2, 0.2)), 0.005, 0.05)
    v_codes = jnp.clip(0.049804688 + 0.9501953 * jax.random.uniform(arg_keys[4], (N_MP, MPB, BLOCK), jnp.float32) ** level_of(arg_keys[4], (N_MP, MPB, BLOCK), ((0, 4), (1, 8)), -0.2, 0.2), 0.049804688, 1.0).astype(jnp.bfloat16)
    v_scale = jnp.clip(jnp.exp(math.log(0.01) - 2.30258502 * jax.random.uniform(arg_keys[5], (N_MP, MPB), jnp.float32) ** level_of(arg_keys[5], (N_MP, MPB), ((0, 4), (1, 8)), -0.2, 0.2)), 0.001, 0.01)
    return dict(grads=grads, master=master, m_codes=m_codes, m_scale=m_scale, v_codes=v_codes, v_scale=v_scale)


def block_code(values):
    scale = (lax.optimization_barrier(jnp.max(jnp.abs(values), axis=-1)) + 1e-06).astype(jnp.bfloat16)
    levels = (values / scale.astype(jnp.float32)[..., None]).astype(jnp.bfloat16)
    return (levels, scale)

def expand(levels, scale):
    return levels.astype(jnp.float32) * scale.astype(jnp.float32)[..., None]

def state_code(values):
    scale = lax.optimization_barrier(jnp.max(jnp.abs(values), axis=-1)) + 1e-06
    return ((values / scale[..., None]).astype(jnp.bfloat16), scale)

def pair_tree(values):
    for level in range(LEVELS - 1):
        pairs = values.reshape((values.shape[0] // 2, 2) + values.shape[1:])
        levels, scale = block_code(pairs[:, 0] + pairs[:, 1])
        values = expand(levels, scale)
    return values[0] + values[1]

def reference(grads, master, m_codes, m_scale, v_codes, v_scale):

    def owner_mean(index):
        shard = (index // N_DP).astype(jnp.int32)
        owner = (index % N_DP).astype(jnp.int32)
        zero = jnp.zeros((), jnp.int32)
        start = (owner * OWNB).astype(jnp.int32)
        piece = lax.dynamic_slice(grads, (zero, shard, start, zero), (N_DP, 1, OWNB, BLOCK))[:, 0]
        levels, scale = block_code(piece.astype(jnp.float32))
        return pair_tree(expand(levels, scale)) / N_DP
    indices = jnp.arange(N_MP * N_DP, dtype=jnp.int32)
    grad_mean = lax.map(owner_mean, indices).reshape(N_MP, MPB, BLOCK)
    moment_one = 0.9 * m_codes.astype(jnp.float32) * m_scale[..., None] + 0.1 * grad_mean
    moment_two = 0.95 * v_codes.astype(jnp.float32) * v_scale[..., None] + 0.05 * grad_mean * grad_mean
    first_fix = 1.0 - 0.9 ** STEP
    second_fix = 1.0 - 0.95 ** STEP
    master_out = master - 0.1 * (moment_one / first_fix) / (jnp.sqrt(moment_two / second_fix) + 1e-08)
    one_code, one_scale = state_code(moment_one)
    two_code, two_scale = state_code(moment_two)
    weights = master_out.astype(jnp.bfloat16)
    return (master_out, one_code, one_scale, two_code, two_scale, weights)
```

```python
import functools
import math

import jax
import jax.numpy as jnp
from jax import lax
from jax.experimental import pallas as pl
from jax.experimental.pallas import tpu as pltpu
from jax.sharding import PartitionSpec as P

STEP = 8
LANES = 128
VMEM_ALL = 67043328
VMEM_GRANT = 60 * 1024 * 1024
MESH = pl.DeviceIdType.MESH

LINE, HALF, DIRECT = 0, 1, 2
ACROSS, SUM, CROSS, UPDATE, SPREAD, PASS = range(6)
PLANS = {}


def unpacked(codes):
    return [
        (c // 100000, c // 1000 % 100, c // 100 % 10, c // 10 % 10, c % 10) for c in codes
    ]


PLANS[4] = (
    (1, 1, 1, 1, 1, 1, 1, 1),
    ((0, HALF), (1, DIRECT), (0, DIRECT), (1, HALF), (0, LINE), (0, DIRECT), (0, LINE), (0, LINE)),
    ((0, LINE), (0, LINE), (0, LINE), (0, LINE), (0, LINE), (0, LINE), (1, HALF), (0, DIRECT)),
    unpacked((
        2000, 101131, 103130, 101021, 103030, 103031, 101110, 101031, 101121, 101011, 101020, 103131, 0, 101120,
        4000, 102030, 102020, 102130, 103020, 102120, 103021, 103121, 103120, 100030, 101111, 5000, 100130, 102010,
        101010, 102110, 104130, 101030, 103110, 100020, 101130, 103111, 104030, 100120, 103011, 201000, 105010, 6000,
        105030, 105130, 302000, 7000, 105120, 100010, 104020, 104120, 301000, 105020, 203000, 105110, 502010, 100110,
        106130, 502110, 107130, 103010, 104110, 106030, 501110, 501010, 104010, 502020, 300000, 106020, 106120, 107030,
        502120, 305000, 107120, 501020, 304000, 303000, 500110, 107020, 505110, 106110, 505010, 106010, 502030, 500010,
        107110, 501120, 107010, 504010, 504110, 505120, 306000, 502130, 501130, 503110, 500020, 500120, 501030, 307000,
        504120, 505020, 500130, 505130, 503010, 507110, 504020, 507010, 406000, 506031, 504130, 505030, 500030, 503120,
        507030, 507130, 506120, 507120, 503020, 504030, 503130, 507020, 506010, 503030, 506020, 506131, 506110, 506111,
        506030, 506130, 506021, 506011, 506121,
    )),
)


def steps_of(k, outer, sums, spreads):
    steps = [] if sums[0] else [(ACROSS, k, 0, 0, 0)]
    for distance in range(outer - 1, 0, -1):
        for other in range(sums[0], -1, -1):
            steps += [(SUM, k, left, distance, other) for left in (0, 1)]
    if sums[0]:
        steps.append((CROSS, k, 0, 0, 0))
    steps.append((UPDATE, k, 0, 0, 0))
    if spreads[0]:
        steps.append((SPREAD, k, 0, 0, 0))
    for distance in range(1, outer):
        for other in range(spreads[0] + 1):
            steps += [(PASS, k, left, distance, other) for left in (0, 1)]
    return steps


def plan_for(outer, owned):
    if outer in PLANS:
        parts, sums, spreads, order = PLANS[outer]
        unit = owned // sum(parts)
        if unit * sum(parts) == owned and unit % 16 == 0:
            return [unit * part for part in parts], sums, spreads, order
    pieces = owned // LANES
    sums = spreads = [(0, LINE)] * pieces
    base = {ACROSS: 0, SUM: 2, CROSS: 3, UPDATE: 4, SPREAD: 5, PASS: 4}

    def rank(step):
        kind, k, _, distance, _ = step
        along = {SUM: (outer - 1 - distance) / outer, PASS: distance}.get(kind, 0)
        return k * (0.25 if kind == ACROSS else 1) + base[kind] + along

    order = sorted((s for k in range(pieces) for s in steps_of(k, outer, sums[k], spreads[k])), key=rank)
    return [LANES] * pieces, sums, spreads, order


def kernel(
    outer, plan, grads, master, m_codes, m_scale, v_codes, v_scale,
    master_new, m_new, ms_new, v_new, vs_new, weights,
    own, xgot, stage, right_got, left_got, total, ms_wide, vs_wide,
    master_in, m_in, v_in, ms_in, vs_in,
    own_sem, state_sem,
    x_send, x_recv, sum_send, right_recv, left_recv, first_send, pass_send, w_recv, a_send, a_recv,
):
    sizes, sums, spreads, order = plan
    pieces = len(sizes)
    starts = [sum(sizes[:k]) for k in range(pieces)]
    owned, width = master.shape[1], master.shape[2]
    replicas = 2 * outer
    f32, bf16 = jnp.float32, jnp.bfloat16
    me = lax.axis_index("dp")
    x = lax.rem(me, 2)
    z = lax.div(me, 2)
    other = z * 2 + 1 - x
    ends = []

    def remote(src, dst, send, recv, device):
        return pltpu.make_async_remote_copy(
            src_ref=src, dst_ref=dst, send_sem=send, recv_sem=recv,
            device_id={"dp": device}, device_id_type=MESH,
        )

    def launch(make, *wanted):
        def run(act):
            if wanted:
                pl.when(functools.reduce(jnp.logical_and, [w() for w in wanted]))(act)
            else:
                act()
        run(lambda: make().start())
        ends.append(lambda: run(lambda: make().wait_send()))

    barrier = pltpu.get_barrier_semaphore()
    pl.semaphore_signal(barrier, inc=1, device_id={"dp": other}, device_id_type=MESH)
    for step in range(1, outer):
        pl.semaphore_signal(
            barrier, inc=1, device_id={"dp": lax.rem(z + step, outer) * 2 + x}, device_id_type=MESH
        )

    def rows_in(k):
        return pl.ds(starts[k], sizes[k])

    own_copies = []
    seen = []
    for step in order:
        if step[1] not in seen:
            seen.append(step[1])
    for k in seen:
        copy = pltpu.make_async_copy(
            grads.at[:, rows_in(k), :], own.at[:, rows_in(k), :], own_sem.at[k]
        )
        copy.start()
        own_copies.append((k, copy))
    own_copies = dict(own_copies)
    scale_copies = [
        pltpu.make_async_copy(m_scale, ms_in, state_sem.at[3]),
        pltpu.make_async_copy(v_scale, vs_in, state_sem.at[4]),
    ]
    state_copies = [
        pltpu.make_async_copy(src, dst, state_sem.at[i])
        for i, (src, dst) in enumerate(((master, master_in), (m_codes, m_in), (v_codes, v_in)))
    ]
    for copy in scale_copies + state_copies:
        copy.start()
    for copy in scale_copies:
        copy.wait()
    for source, wide in ((ms_in, ms_wide), (vs_in, vs_wide)):
        for c in range(owned // LANES):
            span = pl.ds(c * LANES, LANES)
            wide[span, :] = jnp.transpose(jnp.broadcast_to(source[0:1, span], (LANES, LANES)))

    pl.semaphore_wait(barrier, outer)

    loaded = set()

    def load(k):
        if k not in loaded:
            loaded.add(k)
            own_copies[k].wait()

    def column(block):
        return 1 - x if block else x

    def seat(left):
        return outer - 1 - z if left else z

    def at(left, place):
        return outer - 1 - place if left else place

    def got_of(left):
        return (left_got, left_recv) if left else (right_got, right_recv)

    def block_of(k, t, block):
        return own[t * 2 + column(block), rows_in(k), :].astype(f32)

    def x_copy(k, t, src):
        return remote(src, xgot.at[t, rows_in(k), :], x_send.at[k, t], x_recv.at[k, t], other)

    def across(k):
        for step in range(outer):
            def make(step=step):
                t = lax.rem(z + 1 + step, outer)
                return x_copy(k, t, own.at[t * 2 + 1 - x, rows_in(k), :])
            launch(make)

    def x_wait(k, t):
        x_copy(k, t, xgot.at[t, rows_in(k), :]).wait_recv()
        return xgot[t, rows_in(k), :].astype(f32)

    def sum_wait(k, left, slot, block):
        got, recv = got_of(left)
        ref = got.at[slot, block, rows_in(k), :]
        remote(ref, ref, sum_send.at[k, slot, block], recv.at[k, slot, block], other).wait_recv()
        return got[slot, block, rows_in(k), :].astype(f32)

    def partial_sum(k, left, distance, block):
        z_first, form = sums[k]
        got, recv = got_of(left)
        rows = rows_in(k)

        def target():
            return at(left, seat(left) + distance)

        def make(src, slot_of, dest_of):
            t = target()
            return remote(
                src(t), got.at[slot_of(t), block, rows, :], sum_send.at[k, t, block],
                recv.at[k, slot_of(t), block], dest_of(t) * 2 + x,
            )

        def staged(t):
            return stage.at[t, block, rows, :]

        def raw(t):
            return own.at[t * 2 + column(block), rows, :]

        def send(src, slot_of, dest_of, *wanted):
            launch(lambda: make(src, slot_of, dest_of), *wanted)

        def base(t):
            value = block_of(k, t, block)
            return value if z_first else value + x_wait(k, t)

        def fits():
            return seat(left) + distance < outer

        def store_first():
            t = target()
            stage[t, block, rows, :] = base(t).astype(bf16)

        def store_added():
            t = target()
            value = base(t)
            stage[t, block, rows, :] = (value + sum_wait(k, left, t, block)).astype(bf16)

        def neighbour(t):
            return at(left, seat(left) + 1)

        def by_target(t):
            return t

        def by_source(t):
            return z

        if form == DIRECT:
            if not z_first:
                pl.when(fits())(store_first)
            send(raw if z_first else staged, by_source, by_target, fits)
            return
        def opens():
            return seat(left) == 0

        def adds():
            return jnp.logical_and(seat(left) > 0, fits()) if form == LINE else jnp.logical_and(seat(left) == 1, fits())

        def plain():
            return jnp.logical_and(seat(left) > 1, fits())

        adding = distance < outer - 1
        if not z_first:
            pl.when(jnp.logical_and(opens(), fits()))(store_first)
        if adding:
            pl.when(adds())(store_added)
        if form == LINE:
            if z_first:
                send(raw, by_target, neighbour, opens)
                if adding:
                    send(staged, by_target, neighbour, adds)
            else:
                send(staged, by_target, neighbour, fits)
            return
        send(raw if z_first else staged, by_target, neighbour, opens)
        if adding:
            send(staged, by_source, by_target, adds)
            if distance < outer - 2:
                if not z_first:
                    pl.when(plain())(store_first)
                send(raw if z_first else staged, by_source, by_target, plain)

    def gather_sum(k, block):
        z_first, form = sums[k]
        rows = pl.ds(0, sizes[k])
        value = block_of(k, z, block)
        total[rows, :] = value if z_first else value + x_wait(k, z)

        def add(left, slot):
            def run():
                total[rows, :] = total[rows, :] + sum_wait(k, left, slot, block)
            return run

        for left in (0, 1):
            place = seat(left)
            if form == LINE:
                pl.when(place > 0)(add(left, z))
                continue
            if form == HALF:
                pl.when(place == 1)(add(left, z))
            first = 1 if form == HALF else 0
            for apart in range(1, outer - first):
                pl.when(place - apart >= first)(add(left, at(left, place - apart)))
        return total[rows, :]

    def cross(k):
        stage[z, 1, rows_in(k), :] = gather_sum(k, 1).astype(bf16)
        launch(lambda: x_copy(k, z, stage.at[z, 1, rows_in(k), :]))

    def weight_rows(k, source, block):
        start = (source * 2 + column(block)) * owned + starts[k]
        return weights.at[0, pl.ds(pl.multiple_of(start, 16), sizes[k]), :]

    def weight_copy(k, source, block, send, dest):
        rows = weight_rows(k, source, block)
        return remote(rows, rows, send, w_recv.at[k, source, block], dest * 2 + x)

    def weight_across(k, source):
        rows = weight_rows(k, source, 0)
        return remote(rows, rows, a_send.at[k, source], a_recv.at[k, source], other)

    def first_sends(k, block):
        form = spreads[k][1]
        for left in (0, 1):
            for apart in range(1 if form == LINE else outer - 1, 0, -1):
                def wanted(left=left, apart=apart):
                    place = seat(left)
                    if form != HALF:
                        return place + apart < outer
                    inside = place + apart < outer - 1
                    return jnp.logical_or(inside, place == outer - 2) if apart == 1 else inside

                def make(left=left, apart=apart):
                    dest = at(left, seat(left) + apart)
                    return weight_copy(k, z, block, first_send.at[k, dest, block], dest)
                launch(make, wanted)

    def moments(k):
        z_first, _ = sums[k]
        rows = rows_in(k)
        value = gather_sum(k, 0)
        if z_first:
            value = value + x_wait(k, z)
        mean = value * (1.0 / replicas)
        repeat = width // LANES
        ms = jnp.concatenate([ms_wide[rows, :]] * repeat, axis=1)
        vs = jnp.concatenate([vs_wide[rows, :]] * repeat, axis=1)
        one = 0.9 * m_in[0, rows].astype(f32) * ms + 0.1 * mean
        two = 0.95 * v_in[0, rows].astype(f32) * vs + 0.05 * mean * mean
        first_fix = 1.0 - 0.9**STEP
        second_fix = 1.0 - 0.95**STEP
        new = master_in[0, rows] - (0.1 / first_fix) * one / (
            jnp.sqrt(two * (1.0 / second_fix)) + 1e-08
        )
        mine = pl.ds(pl.multiple_of(me * owned + starts[k], 16), sizes[k])
        weights[0, mine, :] = new.astype(bf16)
        if spreads[k][0]:
            launch(lambda: weight_across(k, z))
        first_sends(k, 0)
        if not spreads[k][0]:
            launch(lambda: weight_across(k, z))
        master_new[0, rows] = new
        one_top = jnp.max(jnp.abs(one), axis=-1, keepdims=True) + 1e-06
        two_top = jnp.max(jnp.abs(two), axis=-1, keepdims=True) + 1e-06
        m_new[0, rows] = (one / one_top).astype(bf16)
        v_new[0, rows] = (two / two_top).astype(bf16)
        ms_wide[rows, :] = jnp.broadcast_to(one_top, (sizes[k], LANES))
        vs_wide[rows, :] = jnp.broadcast_to(two_top, (sizes[k], LANES))

    def spread(k):
        rows = weight_rows(k, z, 1)
        remote(rows, rows, a_send.at[k, z], a_recv.at[k, z], other).wait_recv()
        first_sends(k, 1)

    def pass_on(k, left, apart, block):
        z_first, form = spreads[k]

        def source():
            return at(left, seat(left) - apart)

        def arrives():
            return seat(left) - apart >= 0

        def passes():
            if form == LINE:
                return jnp.logical_and(arrives(), seat(left) < outer - 1)
            return jnp.logical_and(arrives(), seat(left) == outer - 2)

        def wait():
            s = source()
            weight_copy(k, s, block, pass_send.at[k, s, block], z).wait_recv()

        def along():
            s = source()
            return weight_copy(k, s, block, pass_send.at[k, s, block], at(left, seat(left) + 1))

        def stays():
            return jnp.logical_and(arrives(), jnp.logical_not(passes()))

        moves = form == LINE and apart < outer - 1 or form == HALF and apart < outer - 1
        if not z_first:
            pl.when(arrives())(wait)
            if moves:
                launch(along, passes)
            launch(lambda: weight_across(k, source()), arrives)
        elif moves:
            pl.when(passes())(wait)
            launch(along, passes)
            ends.append(lambda: pl.when(stays())(wait))
        else:
            ends.append(lambda: pl.when(arrives())(wait))

    updated = 0
    for kind, k, left, distance, block in order:
        load(k)
        if kind == ACROSS:
            across(k)
        elif kind == SUM:
            partial_sum(k, left, distance, block)
        elif kind == CROSS:
            cross(k)
        elif kind == UPDATE:
            if not updated:
                for copy in state_copies:
                    copy.wait()
            updated += 1
            moments(k)
        elif kind == SPREAD:
            spread(k)
        else:
            pass_on(k, left, distance, block)
    for wide, out in ((ms_wide, ms_new), (vs_wide, vs_new)):
        for c in range(owned // LANES):
            span = pl.ds(c * LANES, LANES)
            out[0:1, span] = jnp.transpose(wide[span, :])[0:1, :]
    for end in ends:
        end()
    for k in range(pieces):
        if not spreads[k][0]:
            for source in range(outer):
                weight_across(k, source).wait_recv()


def write_out(*refs):
    sem = refs[-1]
    half = (len(refs) - 1) // 2
    copies = [
        pltpu.make_async_copy(refs[i], refs[half + i], sem.at[i]) for i in range(half)
    ]
    for copy in copies[::-1]:
        copy.start()
    for copy in copies:
        copy.wait()


def per_device(grads, master, m_codes, m_scale, v_codes, v_scale):
    outer = lax.axis_size("dp") // 2
    _, owned, width = master.shape
    plan = plan_for(outer, owned)
    sizes, sums, spreads, _ = plan
    pieces = len(sizes)
    blocks = 1 + max(kind[0] for kind in (*sums, *spreads))
    bf16, f32 = jnp.bfloat16, jnp.float32
    dma = pltpu.SemaphoreType.DMA
    shape = jax.ShapeDtypeStruct
    state = (1, owned, width)
    out_shapes = (
        (state, f32), (state, bf16), ((1, owned), f32),
        (state, bf16), ((1, owned), f32),
        ((1, 2 * outer * owned, width), bf16),
    )
    kept = sum(math.prod(dims) * jnp.dtype(kind).itemsize for dims, kind in out_shapes)
    outs = pl.pallas_call(
        functools.partial(kernel, outer, plan),
        out_shape=tuple(pltpu.VMEM(*each) for each in out_shapes),
        in_specs=[pl.BlockSpec(memory_space=pltpu.HBM)] * 6,
        out_specs=[pl.BlockSpec(memory_space=pltpu.VMEM)] * 6,
        scratch_shapes=[
            pltpu.VMEM((2 * outer, owned, width), bf16),
            pltpu.VMEM((outer, owned, width), bf16),
            pltpu.VMEM((outer, blocks, owned, width), bf16),
            pltpu.VMEM((outer, blocks, owned, width), bf16),
            pltpu.VMEM((outer, blocks, owned, width), bf16),
            pltpu.VMEM((max(sizes), width), f32),
            pltpu.VMEM((owned, LANES), f32), pltpu.VMEM((owned, LANES), f32),
            pltpu.VMEM(state, f32), pltpu.VMEM(state, bf16), pltpu.VMEM(state, bf16),
            pltpu.VMEM((1, owned), f32), pltpu.VMEM((1, owned), f32),
            dma((pieces,)), dma((5,)),
            dma((pieces, outer)), dma((pieces, outer)),
            dma((pieces, outer, blocks)), dma((pieces, outer, blocks)), dma((pieces, outer, blocks)),
            dma((pieces, outer, blocks)), dma((pieces, outer, blocks)), dma((pieces, outer, blocks)),
            dma((pieces, outer)), dma((pieces, outer)),
        ],
        compiler_params=pltpu.CompilerParams(
            collective_id=0, has_side_effects=True,
            vmem_limit_bytes=min(VMEM_GRANT, VMEM_ALL - kept - 2**18),
        ),
    )(grads.reshape(2 * outer, owned, width), master, m_codes, m_scale, v_codes, v_scale)
    return tuple(pl.pallas_call(
        write_out,
        out_shape=tuple(shape(*each) for each in out_shapes),
        in_specs=[pl.BlockSpec(memory_space=pltpu.VMEM)] * 6,
        out_specs=[pl.BlockSpec(memory_space=pl.ANY)] * 6,
        scratch_shapes=[dma((6,))],
        compiler_params=pltpu.CompilerParams(vmem_limit_bytes=2**20),
    )(*[pltpu.with_memory_space_constraint(o, pltpu.VMEM) for o in outs]))


def solution(mesh):
    return jax.shard_map(
        per_device,
        mesh=mesh,
        in_specs=(
            P("dp", "mp", None, None),
            P("mp", "dp", None),
            P("mp", "dp", None),
            P("mp", "dp"),
            P("mp", "dp", None),
            P("mp", "dp"),
        ),
        out_specs=(
            P("mp", "dp", None),
            P("mp", "dp", None),
            P("mp", "dp"),
            P("mp", "dp", None),
            P("mp", "dp"),
            P("mp", None, None),
        ),
        check_vma=False,
    )
```

```python
import functools
import math

import jax
import jax.numpy as jnp
from jax import lax
from jax.experimental import pallas as pl
from jax.experimental.pallas import tpu as pltpu
from jax.sharding import PartitionSpec as P

STEP = 8
LANES = 128
VMEM_ALL = 67043328
VMEM_GRANT = 60 * 1024 * 1024
MESH = pl.DeviceIdType.MESH

LINE, HALF, DIRECT = 0, 1, 2
ACROSS, SUM, CROSS, UPDATE, SPREAD, PASS, OVER = range(7)
CHUNK = 64
PLANS = {}


def unpacked(codes):
    return [
        (c // 100000, c // 1000 % 100, c // 100 % 10, c // 10 % 10, c % 10) for c in codes
    ]


PLANS[4] = (
    (1, 1, 1, 1, 1, 1, 1, 1),
    ((0, LINE), (0, LINE), (0, LINE), (1, HALF), (0, LINE), (0, LINE), (0, LINE), (0, LINE)),
    ((1, LINE), (0, HALF), (0, HALF), (0, LINE), (1, LINE), (0, LINE), (0, LINE), (0, LINE)),
    (
        unpacked((
            30, 1030, 103010, 103021, 103020, 6030, 103031, 4030, 20, 103030, 1020, 103011, 5030, 100030,
            2030, 101030, 6020, 7030, 104030, 4020, 100020, 10, 101020, 106030, 105030, 5020, 203000, 0,
            106020, 1010, 107030, 2020, 104020, 102030, 6010, 100010, 1000, 303000, 7020, 105020, 4010, 6000,
            101010, 4000, 102020, 300000, 5010, 106010, 2010, 301000, 5000, 107020, 7010, 104010, 2000, 7000,
            304000, 306000, 105010, 102010, 603110, 305000, 107010, 601110, 302000, 603130, 307000, 606120, 606110, 400000,
            601130, 404000, 605110, 606130, 605120, 605130, 602120, 603120, 602130, 601120, 602110, 607130, 607120, 607110,
        )),
        unpacked((
            30, 1030, 103110, 103111, 6030, 4030, 0, 20, 5030, 1000, 103011, 10, 103010, 1020,
            103021, 103020, 2030, 203000, 6000, 101020, 6020, 100020, 1010, 104020, 7030, 100010, 4000, 101010,
            303000, 101110, 4020, 105020, 100110, 6010, 106020, 4010, 106010, 5000, 5020, 107020, 503110, 2000,
            300000, 104110, 2020, 102020, 104010, 106110, 5010, 7000, 503010, 7020, 301000, 105110, 500110, 2010,
            105010, 7010, 102110, 306000, 500010, 102010, 503120, 603110, 501110, 304000, 107110, 107010, 506110, 606110,
            506010, 606010, 603010, 305000, 500120, 302000, 501120, 601110, 505010, 605010, 307000, 506120, 504010, 601010,
            505110, 605110, 505120, 602010, 502110, 602110, 507010, 502120, 400000, 504120, 606120, 500011, 507110, 504011,
            602120, 507120, 605120, 500111, 603120, 404000, 500121, 601120, 504121, 607010, 607110, 504110, 504111, 607120,
        )),
        unpacked((
            0, 1000, 103010, 103011, 6000, 4000, 30, 10, 5000, 1030, 103111, 20, 103110, 1010,
            103121, 103120, 2000, 203000, 6030, 101120, 6010, 100120, 1020, 104120, 7000, 100110, 4030, 101110,
            303000, 101010, 4010, 105120, 100010, 6020, 106120, 4020, 106110, 5030, 5010, 107120, 503010, 2030,
            300000, 104010, 2010, 102120, 104110, 106010, 5020, 7030, 503110, 7010, 301000, 105010, 500010, 2020,
            105110, 7020, 102010, 306000, 500110, 102110, 503020, 603010, 501010, 304000, 107010, 107110, 506010, 606010,
            506110, 606110, 603110, 305000, 500020, 302000, 501020, 601010, 505110, 605110, 307000, 506020, 504110, 601110,
            505010, 605010, 505020, 602110, 502010, 602010, 507110, 502020, 400000, 504020, 606020, 500111, 507010, 504111,
            602020, 507020, 605020, 500011, 603020, 404000, 500021, 601020, 504021, 607110, 607010, 504010, 504011, 607020,
        )),
        unpacked((
            0, 1000, 103110, 103121, 103120, 6000, 103131, 4000, 10, 103130, 1010, 103111, 5000, 100130,
            2000, 101130, 6010, 7000, 104130, 4010, 100120, 20, 101120, 106130, 105130, 5010, 203000, 30,
            106120, 1020, 107130, 2010, 104120, 102130, 6020, 100110, 1030, 303000, 7010, 105120, 4020, 6030,
            101110, 4030, 102120, 300000, 5020, 106110, 2020, 301000, 5030, 107120, 7020, 104110, 2030, 7030,
            304000, 306000, 105110, 102110, 603010, 305000, 107110, 601010, 302000, 603030, 307000, 606020, 606010, 400000,
            601030, 404000, 605010, 606030, 605020, 605030, 602020, 603020, 602030, 601020, 602010, 607030, 607020, 607010,
        )),
    ),
)


def plan_for(outer, owned):
    if outer in PLANS:
        parts, sums, spreads, orders = PLANS[outer]
        unit = owned // sum(parts)
        if unit * sum(parts) == owned and unit % 16 == 0:
            return [unit * part for part in parts], sums, spreads, orders
    orders = []
    for z in range(outer):
        order = [(ACROSS, 0, 0, (z + 1 + step) % outer, 0) for step in range(outer)]
        for distance in range(outer - 1, 0, -1):
            order += [
                (SUM, 0, left, distance, 0) for left in (0, 1)
                if (z - distance >= 0 if left else z + distance < outer)
            ]
        order.append((UPDATE, 0, 0, 0, 0))
        for distance in range(1, outer):
            for left in (0, 1):
                if z + distance < outer if left else z - distance >= 0:
                    if z > 0 if left else z < outer - 1:
                        order.append((PASS, 0, left, distance, 0))
                    order.append((OVER, 0, left, distance, 0))
        orders.append(order)
    return [owned], [(0, LINE)], [(0, LINE)], orders


def kernel(
    outer, plan, grads, master, m_codes, m_scale, v_codes, v_scale,
    master_new, m_new, ms_new, v_new, vs_new, weights,
    own, xgot, stage, right_got, left_got, ms_wide, vs_wide,
    master_in, m_in, v_in, ms_in, vs_in,
    own_sem, state_sem,
    x_send, x_recv, sum_send, right_recv, left_recv, first_send, pass_send, w_recv, a_send, a_recv,
):
    sizes, sums, spreads, orders = plan
    pieces = len(sizes)
    starts = [sum(sizes[:k]) for k in range(pieces)]
    owned, width = master.shape[1], master.shape[2]
    replicas = 2 * outer
    f32, bf16 = jnp.float32, jnp.bfloat16
    me = lax.axis_index("dp")
    x = lax.rem(me, 2)
    place = lax.div(me, 2)
    other = place * 2 + 1 - x

    barrier = pltpu.get_barrier_semaphore()
    pl.semaphore_signal(barrier, inc=1, device_id={"dp": other}, device_id_type=MESH)
    for step in range(1, outer):
        pl.semaphore_signal(
            barrier, inc=1, device_id={"dp": lax.rem(place + step, outer) * 2 + x}, device_id_type=MESH
        )

    def rows_in(k):
        return pl.ds(starts[k], sizes[k])

    own_copies = [
        pltpu.make_async_copy(grads.at[:, rows_in(k), :], own.at[:, rows_in(k), :], own_sem.at[k])
        for k in range(pieces)
    ]
    scale_copies = [
        pltpu.make_async_copy(m_scale, ms_in, state_sem.at[3]),
        pltpu.make_async_copy(v_scale, vs_in, state_sem.at[4]),
    ]
    state_copies = [
        pltpu.make_async_copy(src, dst, state_sem.at[i])
        for i, (src, dst) in enumerate(((master, master_in), (m_codes, m_in), (v_codes, v_in)))
    ]
    for copy in own_copies + scale_copies + state_copies:
        copy.start()
    for copy in scale_copies:
        copy.wait()
    for source, wide in ((ms_in, ms_wide), (vs_in, vs_wide)):
        for c in range(owned // LANES):
            span = pl.ds(c * LANES, LANES)
            wide[span, :] = jnp.transpose(jnp.broadcast_to(source[0:1, span], (LANES, LANES)))
    for copy in own_copies + state_copies:
        copy.wait()
    pl.semaphore_wait(barrier, outer)

    def remote(src, dst, send, recv, device):
        return pltpu.make_async_remote_copy(
            src_ref=src, dst_ref=dst, send_sem=send, recv_sem=recv,
            device_id={"dp": device}, device_id_type=MESH,
        )

    def column(block):
        return 1 - x if block else x

    def in_rows(k, body):
        chunk = min(CHUNK, sizes[k])
        count = sizes[k] // chunk
        if count <= 2 and count * chunk == sizes[k]:
            for c in range(count):
                body(pl.ds(starts[k] + c * chunk, chunk))
        elif count * chunk == sizes[k]:
            lax.fori_loop(
                0, count, lambda c, _: body(pl.ds(pl.multiple_of(starts[k] + c * chunk, 16), chunk)), None
            )
        else:
            body(rows_in(k))

    def program(z):
        started = []
        taken = set()

        def launch(copy):
            copy.start()
            started.append(copy)

        def seat(left):
            return outer - 1 - z if left else z

        def at(left, number):
            return outer - 1 - number if left else number

        def x_copy(k, t, src):
            return remote(src, xgot.at[t, rows_in(k), :], x_send.at[k, t], x_recv.at[k, t], other)

        def x_wait(k, t):
            x_copy(k, t, xgot.at[t, rows_in(k), :]).wait_recv()

        def across(k, t):
            launch(x_copy(k, t, own.at[t * 2 + 1 - x, rows_in(k), :]))

        def got_of(left):
            return (left_got, left_recv) if left else (right_got, right_recv)

        def sum_wait(k, left, slot, block):
            got, recv = got_of(left)
            ref = got.at[slot, block, rows_in(k), :]
            remote(ref, ref, sum_send.at[k, slot, block], recv.at[k, slot, block], other).wait_recv()

        def add_up(k, t, block, terms, rows):
            total = own[t * 2 + column(block), rows, :].astype(f32)
            if not sums[k][0]:
                total = total + xgot[t, rows, :].astype(f32)
            for left, slot in terms:
                total = total + got_of(left)[0][slot, block, rows, :].astype(f32)
            return total

        def partial_sum(k, left, distance, block):
            z_first, form = sums[k]
            got, recv = got_of(left)
            seated = seat(left)
            t = at(left, seated + distance)
            adds = form == LINE and seated > 0 or form == HALF and seated == 1
            hops = form == LINE or form == HALF and seated == 0
            slot = t if hops else z
            dest = at(left, seated + 1) if hops else t
            if z_first and not adds:
                src = own.at[t * 2 + column(block), rows_in(k), :]
            else:
                if not z_first:
                    x_wait(k, t)
                if adds:
                    sum_wait(k, left, t, block)

                def body(rows):
                    total = add_up(k, t, block, [(left, t)] if adds else [], rows)
                    stage[t, block, rows, :] = total.astype(bf16)
                in_rows(k, body)
                src = stage.at[t, block, rows_in(k), :]
            launch(remote(
                src, got.at[slot, block, rows_in(k), :], sum_send.at[k, t, block],
                recv.at[k, slot, block], dest * 2 + x,
            ))

        def arrived(k, block):
            form = sums[k][1]
            terms = []
            for left in (0, 1):
                seated = seat(left)
                if seated == 0:
                    continue
                if form == LINE or form == HALF and seated == 1:
                    terms.append((left, z))
                else:
                    terms += [(left, at(left, s)) for s in range(1 if form == HALF else 0, seated)]
            if not sums[k][0]:
                x_wait(k, z)
            for left, slot in terms:
                sum_wait(k, left, slot, block)
            return terms

        def cross(k):
            terms = arrived(k, 1)

            def body(rows):
                stage[z, 1, rows, :] = add_up(k, z, 1, terms, rows).astype(bf16)
            in_rows(k, body)
            launch(x_copy(k, z, stage.at[z, 1, rows_in(k), :]))

        def weight_rows(k, source, block):
            start = (source * 2 + column(block)) * owned + starts[k]
            return weights.at[0, pl.ds(pl.multiple_of(start, 16), sizes[k]), :]

        def weight_copy(k, source, block, send, dest):
            rows = weight_rows(k, source, block)
            return remote(rows, rows, send, w_recv.at[k, source, block], dest * 2 + x)

        def weight_wait(k, source, block):
            if (k, source, block) not in taken:
                taken.add((k, source, block))
                weight_copy(k, source, block, pass_send.at[k, source, block], z).wait_recv()

        def weight_over(k, source):
            rows = weight_rows(k, source, 0)
            return remote(rows, rows, a_send.at[k, source], a_recv.at[k, source], other)

        def first_sends(k, block):
            form = spreads[k][1]
            for left in (0, 1):
                seated = seat(left)
                last = outer - 1
                if seated == last:
                    continue
                if form == LINE or form == HALF and seated == last - 1:
                    dests = [seated + 1]
                else:
                    dests = range(last if form == DIRECT else last - 1, seated, -1)
                for number in dests:
                    dest = at(left, number)
                    launch(weight_copy(k, z, block, first_send.at[k, dest, block], dest))

        def update(k):
            terms = arrived(k, 0)
            if sums[k][0]:
                x_wait(k, z)
            repeat = width // LANES
            first_fix = 1.0 - 0.9**STEP
            second_fix = 1.0 - 0.95**STEP

            def body(rows):
                value = add_up(k, z, 0, terms, rows)
                if sums[k][0]:
                    value = value + xgot[z, rows, :].astype(f32)
                mean = value * (1.0 / replicas)
                ms = jnp.concatenate([ms_wide[rows, :]] * repeat, axis=1)
                vs = jnp.concatenate([vs_wide[rows, :]] * repeat, axis=1)
                one = 0.9 * m_in[0, rows].astype(f32) * ms + 0.1 * mean
                two = 0.95 * v_in[0, rows].astype(f32) * vs + 0.05 * mean * mean
                new = master_in[0, rows] - (0.1 / first_fix) * one / (
                    jnp.sqrt(two * (1.0 / second_fix)) + 1e-08
                )
                mine = pl.ds(pl.multiple_of(me * owned + rows.start, 16), rows.size)
                weights[0, mine, :] = new.astype(bf16)
                master_new[0, rows] = new
                one_top = jnp.max(jnp.abs(one), axis=-1, keepdims=True) + 1e-06
                two_top = jnp.max(jnp.abs(two), axis=-1, keepdims=True) + 1e-06
                m_new[0, rows] = (one / one_top).astype(bf16)
                v_new[0, rows] = (two / two_top).astype(bf16)
                ms_wide[rows, :] = jnp.broadcast_to(one_top, (rows.size, LANES))
                vs_wide[rows, :] = jnp.broadcast_to(two_top, (rows.size, LANES))
            in_rows(k, body)
            if spreads[k][0]:
                launch(weight_over(k, z))
            first_sends(k, 0)
            if not spreads[k][0]:
                launch(weight_over(k, z))

        def spread(k):
            weight_over(k, z).wait_recv()
            first_sends(k, 1)

        def pass_on(k, left, apart, block):
            source = at(left, seat(left) - apart)
            weight_wait(k, source, block)
            launch(weight_copy(
                k, source, block, pass_send.at[k, source, block], at(left, seat(left) + 1)
            ))

        def over(k, left, apart):
            source = at(left, seat(left) - apart)
            weight_wait(k, source, 0)
            launch(weight_over(k, source))

        for kind, k, left, distance, block in orders[z]:
            if kind == ACROSS:
                across(k, distance)
            elif kind == SUM:
                partial_sum(k, left, distance, block)
            elif kind == CROSS:
                cross(k)
            elif kind == UPDATE:
                update(k)
            elif kind == SPREAD:
                spread(k)
            elif kind == PASS:
                pass_on(k, left, distance, block)
            else:
                over(k, left, distance)
        for wide, out in ((ms_wide, ms_new), (vs_wide, vs_new)):
            for c in range(owned // LANES):
                span = pl.ds(c * LANES, LANES)
                out[0:1, span] = jnp.transpose(wide[span, :])[0:1, :]
        for copy in started:
            copy.wait_send()
        for k in range(pieces):
            for source in range(outer):
                for block in range(1 + spreads[k][0]):
                    if source != z:
                        weight_wait(k, source, block)
                if not spreads[k][0]:
                    weight_over(k, source).wait_recv()

    for z in range(outer):
        pl.when(place == z)(functools.partial(program, z))


def write_out(*refs):
    sem = refs[-1]
    half = (len(refs) - 1) // 2
    copies = [
        pltpu.make_async_copy(refs[i], refs[half + i], sem.at[i]) for i in range(half)
    ]
    for copy in copies[::-1]:
        copy.start()
    for copy in copies:
        copy.wait()


def per_device(grads, master, m_codes, m_scale, v_codes, v_scale):
    outer = lax.axis_size("dp") // 2
    _, owned, width = master.shape
    plan = plan_for(outer, owned)
    sizes, sums, spreads, _ = plan
    pieces = len(sizes)
    blocks = 1 + max(kind[0] for kind in (*sums, *spreads))
    bf16, f32 = jnp.bfloat16, jnp.float32
    dma = pltpu.SemaphoreType.DMA
    shape = jax.ShapeDtypeStruct
    state = (1, owned, width)
    out_shapes = (
        (state, f32), (state, bf16), ((1, owned), f32),
        (state, bf16), ((1, owned), f32),
        ((1, 2 * outer * owned, width), bf16),
    )
    kept = sum(math.prod(dims) * jnp.dtype(kind).itemsize for dims, kind in out_shapes)
    outs = pl.pallas_call(
        functools.partial(kernel, outer, plan),
        out_shape=tuple(pltpu.VMEM(*each) for each in out_shapes),
        in_specs=[pl.BlockSpec(memory_space=pltpu.HBM)] * 6,
        out_specs=[pl.BlockSpec(memory_space=pltpu.VMEM)] * 6,
        scratch_shapes=[
            pltpu.VMEM((2 * outer, owned, width), bf16),
            pltpu.VMEM((outer, owned, width), bf16),
            pltpu.VMEM((outer, blocks, owned, width), bf16),
            pltpu.VMEM((outer, blocks, owned, width), bf16),
            pltpu.VMEM((outer, blocks, owned, width), bf16),
            pltpu.VMEM((owned, LANES), f32), pltpu.VMEM((owned, LANES), f32),
            pltpu.VMEM(state, f32), pltpu.VMEM(state, bf16), pltpu.VMEM(state, bf16),
            pltpu.VMEM((1, owned), f32), pltpu.VMEM((1, owned), f32),
            dma((pieces,)), dma((5,)),
            dma((pieces, outer)), dma((pieces, outer)),
            dma((pieces, outer, blocks)), dma((pieces, outer, blocks)), dma((pieces, outer, blocks)),
            dma((pieces, outer, blocks)), dma((pieces, outer, blocks)), dma((pieces, outer, blocks)),
            dma((pieces, outer)), dma((pieces, outer)),
        ],
        compiler_params=pltpu.CompilerParams(
            collective_id=0, has_side_effects=True,
            vmem_limit_bytes=min(VMEM_GRANT, VMEM_ALL - kept - 2**18),
        ),
    )(grads.reshape(2 * outer, owned, width), master, m_codes, m_scale, v_codes, v_scale)
    return tuple(pl.pallas_call(
        write_out,
        out_shape=tuple(shape(*each) for each in out_shapes),
        in_specs=[pl.BlockSpec(memory_space=pltpu.VMEM)] * 6,
        out_specs=[pl.BlockSpec(memory_space=pl.ANY)] * 6,
        scratch_shapes=[dma((6,))],
        compiler_params=pltpu.CompilerParams(vmem_limit_bytes=2**20),
    )(*[pltpu.with_memory_space_constraint(o, pltpu.VMEM) for o in outs]))


def solution(mesh):
    return jax.shard_map(
        per_device,
        mesh=mesh,
        in_specs=(
            P("dp", "mp", None, None),
            P("mp", "dp", None),
            P("mp", "dp", None),
            P("mp", "dp"),
            P("mp", "dp", None),
            P("mp", "dp"),
        ),
        out_specs=(
            P("mp", "dp", None),
            P("mp", "dp", None),
            P("mp", "dp"),
            P("mp", "dp", None),
            P("mp", "dp"),
            P("mp", None, None),
        ),
        check_vma=False,
    )
```

```python
import functools
import math

import jax
import jax.numpy as jnp
from jax import lax
from jax.experimental import pallas as pl
from jax.experimental.pallas import tpu as pltpu
from jax.sharding import PartitionSpec as P

STEP = 8
LANES = 128
VMEM_ALL = 67043328
VMEM_GRANT = 60 * 1024 * 1024
MESH = pl.DeviceIdType.MESH

LINE, HALF, DIRECT = 0, 1, 2
ACROSS, SUM, CROSS, UPDATE, SPREAD, PASS, OVER = range(7)
CHUNK = 64
PLANS = {}


def unpacked(codes):
    return [
        (c // 100000, c // 1000 % 100, c // 100 % 10, c // 10 % 10, c % 10) for c in codes
    ]


PLANS[4] = (
    (3, 3, 3, 3, 2, 2),
    (
        (
            ((0, LINE), (0, DIRECT), (0, HALF), (0, HALF), (1, LINE), (1, LINE)),
            ((0, LINE), (0, LINE), (1, HALF), (0, LINE), (0, HALF), (0, HALF)),
            (
                unpacked((
                    30, 1030, 104010, 104031, 104030, 1020, 104021, 104020, 2030, 104011, 3030, 100030, 1010,
                    101030, 2020, 101020, 3020, 105031, 2010, 103030, 105030, 3010, 101010, 1000, 105021, 204000,
                    2000, 103020, 3000, 105020, 20, 103010, 105011, 301000, 10, 105010, 0, 303000, 100020,
                    102030, 601110, 100010, 205000, 102020, 604110, 604120, 102010, 300000, 305000, 304000, 603110, 601130,
                    601120, 302000, 603120, 603130, 605110, 605130, 600110, 402000, 600120, 605120, 604130, 600130,
                )),
                unpacked((
                    30, 1030, 1000, 1020, 2030, 3030, 104021, 101020, 104020, 2000, 104011, 101110, 2020,
                    104010, 104111, 3000, 100020, 3020, 104110, 101010, 204000, 1010, 102110, 2010, 103020, 105021,
                    3010, 103110, 105020, 0, 304000, 301000, 103010, 20, 105011, 105111, 105010, 10, 105110,
                    504110, 100110, 501010, 601010, 501110, 601110, 303000, 503010, 603010, 205000, 100010, 501120, 102020,
                    503110, 603110, 102010, 601120, 503120, 603120, 300000, 305000, 500010, 505120, 302000, 605010, 504120,
                    605120, 500110, 505110, 605110, 600010, 500120, 600110, 402000, 502110, 604110, 604010, 502120, 600120,
                    604120, 502121, 502111,
                )),
                unpacked((
                    0, 1000, 1030, 1010, 2000, 3000, 104121, 101120, 104120, 2030, 104111, 101010, 2010,
                    104110, 104011, 3030, 100120, 3010, 104010, 101110, 204000, 1020, 102010, 2020, 103120, 105121,
                    3020, 103010, 105120, 30, 304000, 301000, 103110, 10, 105111, 105011, 105110, 20, 105010,
                    504010, 100010, 501110, 601110, 501010, 601010, 303000, 503110, 603110, 205000, 100110, 501020, 102120,
                    503010, 603010, 102110, 601020, 503020, 603020, 300000, 305000, 500110, 505020, 302000, 605110, 504020,
                    605020, 500010, 505010, 605010, 600110, 500020, 600010, 402000, 502010, 604010, 604110, 502020, 600020,
                    604020, 502021, 502011,
                )),
                unpacked((
                    0, 1000, 104110, 104131, 104130, 1010, 104121, 104120, 2000, 104111, 3000, 100130, 1020,
                    101130, 2010, 101120, 3010, 105131, 2020, 103130, 105130, 3020, 101110, 1030, 105121, 204000,
                    2030, 103120, 3030, 105120, 10, 103110, 105111, 301000, 20, 105110, 30, 303000, 100120,
                    102130, 601010, 100110, 205000, 102120, 604010, 604020, 102110, 300000, 305000, 304000, 603010, 601030,
                    601020, 302000, 603020, 603030, 605010, 605030, 600010, 402000, 600020, 605020, 604030, 600030,
                )),
            ),
        ),
    ),
)


def plan_for(outer, owned):
    if outer in PLANS:
        parts, turns = PLANS[outer]
        unit = owned // sum(parts)
        if unit * sum(parts) == owned and unit % 16 == 0:
            return [unit * part for part in parts], turns
    orders = []
    for z in range(outer):
        order = [(ACROSS, 0, 0, (z + 1 + step) % outer, 0) for step in range(outer)]
        for distance in range(outer - 1, 0, -1):
            order += [
                (SUM, 0, left, distance, 0) for left in (0, 1)
                if (z - distance >= 0 if left else z + distance < outer)
            ]
        order.append((UPDATE, 0, 0, 0, 0))
        for distance in range(1, outer):
            for left in (0, 1):
                if z + distance < outer if left else z - distance >= 0:
                    if z > 0 if left else z < outer - 1:
                        order.append((PASS, 0, left, distance, 0))
                    order.append((OVER, 0, left, distance, 0))
        orders.append(order)
    return [owned], [([(0, LINE)], [(0, LINE)], orders)]


def kernel(
    outer, plan, grads, master, m_codes, m_scale, v_codes, v_scale,
    master_new, m_new, ms_new, v_new, vs_new, weights,
    own, xgot, stage, right_got, left_got, one_kept, two_kept, ms_wide, vs_wide,
    master_in, m_in, v_in, ms_in, vs_in,
    own_sem, state_sem,
    x_send, x_recv, sum_send, right_recv, left_recv, first_send, pass_send, w_recv, a_send, a_recv,
):
    sizes, turns = plan
    pieces = len(sizes)
    starts = [sum(sizes[:k]) for k in range(pieces)]
    owned, width = master.shape[1], master.shape[2]
    replicas = 2 * outer
    f32, bf16 = jnp.float32, jnp.bfloat16
    me = lax.axis_index("dp")
    x = lax.rem(me, 2)
    place = lax.div(me, 2)
    other = place * 2 + 1 - x

    forms = [form for sums, spreads, _ in turns for _, form in (*sums, *spreads)]
    reach = outer - 1 if DIRECT in forms else max(1, outer - 2) if HALF in forms else 1
    barrier = pltpu.get_barrier_semaphore()
    pl.semaphore_signal(barrier, inc=1, device_id={"dp": other}, device_id_type=MESH)
    for step in range(1, reach + 1):
        for near, inside in ((place - step, place >= step), (place + step, place + step < outer)):
            pl.when(inside)(functools.partial(
                pl.semaphore_signal, barrier, inc=1, device_id={"dp": near * 2 + x}, device_id_type=MESH
            ))

    def rows_in(k):
        return pl.ds(starts[k], sizes[k])

    own_copies = [
        pltpu.make_async_copy(grads.at[:, rows_in(k), :], own.at[:, rows_in(k), :], own_sem.at[k])
        for k in range(pieces)
    ]
    state_copies = [
        pltpu.make_async_copy(src, dst, state_sem.at[i])
        for i, (src, dst) in enumerate((
            (master, master_in), (m_codes, m_in), (v_codes, v_in), (m_scale, ms_in), (v_scale, vs_in),
        ))
    ]
    uses = list(dict.fromkeys(step[1] for step in turns[0][2][0]))
    for k in uses:
        own_copies[k].start()
    for copy in state_copies:
        copy.start()
    near = sum(
        (place >= step).astype(jnp.int32) + (place + step < outer).astype(jnp.int32)
        for step in range(1, reach + 1)
    )
    pl.semaphore_wait(barrier, 1 + near)

    def remote(src, dst, send, recv, device):
        return pltpu.make_async_remote_copy(
            src_ref=src, dst_ref=dst, send_sem=send, recv_sem=recv,
            device_id={"dp": device}, device_id_type=MESH,
        )

    def column(block):
        return 1 - x if block else x

    def in_rows(k, body):
        chunk = min(CHUNK, sizes[k])
        count = sizes[k] // chunk
        if count <= 2 and count * chunk == sizes[k]:
            for c in range(count):
                body(pl.ds(starts[k] + c * chunk, chunk))
        elif count * chunk == sizes[k]:
            lax.fori_loop(
                0, count, lambda c, _: body(pl.ds(pl.multiple_of(starts[k] + c * chunk, 16), chunk)), None
            )
        else:
            body(rows_in(k))

    def program(turn, z):
        sums, spreads, orders = turns[turn]
        started = []
        taken = set()
        loaded = set()

        def load(k):
            if k not in loaded:
                loaded.add(k)
                own_copies[k].wait()

        def load_state():
            for copy in state_copies:
                copy.wait()
            for source, wide in ((ms_in, ms_wide), (vs_in, vs_wide)):
                for c in range(owned // LANES):
                    span = pl.ds(c * LANES, LANES)
                    wide[span, :] = jnp.transpose(jnp.broadcast_to(source[0:1, span], (LANES, LANES)))

        def launch(copy):
            copy.start()
            started.append(copy)

        def seat(left):
            return outer - 1 - z if left else z

        def at(left, number):
            return outer - 1 - number if left else number

        def x_copy(k, t, src):
            return remote(src, xgot.at[t, rows_in(k), :], x_send.at[k, t], x_recv.at[k, t], other)

        def x_wait(k, t):
            x_copy(k, t, xgot.at[t, rows_in(k), :]).wait_recv()

        def across(k, t):
            launch(x_copy(k, t, own.at[t * 2 + 1 - x, rows_in(k), :]))

        def got_of(left):
            return (left_got, left_recv) if left else (right_got, right_recv)

        def sum_wait(k, left, slot, block):
            got, recv = got_of(left)
            ref = got.at[slot, block, rows_in(k), :]
            remote(ref, ref, sum_send.at[k, slot, block], recv.at[k, slot, block], other).wait_recv()

        def add_up(k, t, block, terms, rows):
            total = own[t * 2 + column(block), rows, :].astype(f32)
            if not sums[k][0]:
                total = total + xgot[t, rows, :].astype(f32)
            for left, slot in terms:
                total = total + got_of(left)[0][slot, block, rows, :].astype(f32)
            return total

        def partial_sum(k, left, distance, block):
            z_first, form = sums[k]
            got, recv = got_of(left)
            seated = seat(left)
            t = at(left, seated + distance)
            adds = form == LINE and seated > 0 or form == HALF and seated == 1
            hops = form == LINE or form == HALF and seated == 0
            slot = t if hops else z
            dest = at(left, seated + 1) if hops else t
            if z_first and not adds:
                src = own.at[t * 2 + column(block), rows_in(k), :]
            else:
                if not z_first:
                    x_wait(k, t)
                if adds:
                    sum_wait(k, left, t, block)

                def body(rows):
                    if adds and z_first:
                        total = own[t * 2 + column(block), rows, :] + got[t, block, rows, :]
                    elif adds:
                        total = add_up(k, t, block, [(left, t)], rows)
                    else:
                        total = own[t * 2 + column(block), rows, :] + xgot[t, rows, :]
                    stage[t, block, rows, :] = total.astype(bf16)
                in_rows(k, body)
                src = stage.at[t, block, rows_in(k), :]
            launch(remote(
                src, got.at[slot, block, rows_in(k), :], sum_send.at[k, t, block],
                recv.at[k, slot, block], dest * 2 + x,
            ))

        def arrived(k, block):
            form = sums[k][1]
            terms = []
            for left in (0, 1):
                seated = seat(left)
                if seated == 0:
                    continue
                if form == LINE or form == HALF and seated == 1:
                    terms.append((left, z))
                else:
                    terms += [(left, at(left, s)) for s in range(1 if form == HALF else 0, seated)]
            if not sums[k][0]:
                x_wait(k, z)
            for left, slot in terms:
                sum_wait(k, left, slot, block)
            return terms

        def cross(k):
            terms = arrived(k, 1)

            def body(rows):
                stage[z, 1, rows, :] = add_up(k, z, 1, terms, rows).astype(bf16)
            in_rows(k, body)
            launch(x_copy(k, z, stage.at[z, 1, rows_in(k), :]))

        def weight_rows(k, source, block):
            start = (source * 2 + column(block)) * owned + starts[k]
            return weights.at[0, pl.ds(pl.multiple_of(start, 16), sizes[k]), :]

        def weight_copy(k, source, block, send, dest):
            rows = weight_rows(k, source, block)
            return remote(rows, rows, send, w_recv.at[k, source, block], dest * 2 + x)

        def weight_wait(k, source, block):
            if (k, source, block) not in taken:
                taken.add((k, source, block))
                weight_copy(k, source, block, pass_send.at[k, source, block], z).wait_recv()

        def weight_over(k, source):
            rows = weight_rows(k, source, 0)
            return remote(rows, rows, a_send.at[k, source], a_recv.at[k, source], other)

        def first_sends(k, block):
            form = spreads[k][1]
            for left in (0, 1):
                seated = seat(left)
                last = outer - 1
                if seated == last:
                    continue
                if form == LINE or form == HALF and seated == last - 1:
                    dests = [seated + 1]
                else:
                    dests = range(last if form == DIRECT else last - 1, seated, -1)
                for number in dests:
                    dest = at(left, number)
                    launch(weight_copy(k, z, block, first_send.at[k, dest, block], dest))

        def update(k):
            terms = arrived(k, 0)
            if sums[k][0]:
                x_wait(k, z)
            repeat = width // LANES
            first_fix = 1.0 - 0.9**STEP
            second_fix = 1.0 - 0.95**STEP

            def body(rows):
                value = add_up(k, z, 0, terms, rows)
                if sums[k][0]:
                    value = value + xgot[z, rows, :].astype(f32)
                mean = value * (1.0 / replicas)
                ms = jnp.concatenate([ms_wide[rows, :]] * repeat, axis=1)
                vs = jnp.concatenate([vs_wide[rows, :]] * repeat, axis=1)
                one = 0.9 * m_in[0, rows].astype(f32) * ms + 0.1 * mean
                two = 0.95 * v_in[0, rows].astype(f32) * vs + 0.05 * mean * mean
                new = master_in[0, rows] - (0.1 / first_fix) * one / (
                    jnp.sqrt(two * (1.0 / second_fix)) + 1e-08
                )
                mine = pl.ds(pl.multiple_of(me * owned + rows.start, 16), rows.size)
                weights[0, mine, :] = new.astype(bf16)
                master_new[0, rows] = new
                one_kept[rows, :] = one
                two_kept[rows, :] = two

            def code(rows):
                one = one_kept[rows, :]
                two = two_kept[rows, :]
                one_top = jnp.max(jnp.abs(one), axis=-1, keepdims=True) + 1e-06
                two_top = jnp.max(jnp.abs(two), axis=-1, keepdims=True) + 1e-06
                m_new[0, rows] = (one / one_top).astype(bf16)
                v_new[0, rows] = (two / two_top).astype(bf16)
                ms_wide[rows, :] = jnp.broadcast_to(one_top, (rows.size, LANES))
                vs_wide[rows, :] = jnp.broadcast_to(two_top, (rows.size, LANES))
            in_rows(k, body)
            if spreads[k][0]:
                launch(weight_over(k, z))
            first_sends(k, 0)
            if not spreads[k][0]:
                launch(weight_over(k, z))
            in_rows(k, code)

        def spread(k):
            weight_over(k, z).wait_recv()
            first_sends(k, 1)

        def pass_on(k, left, apart, block):
            source = at(left, seat(left) - apart)
            weight_wait(k, source, block)
            launch(weight_copy(
                k, source, block, pass_send.at[k, source, block], at(left, seat(left) + 1)
            ))

        def over(k, left, apart):
            source = at(left, seat(left) - apart)
            weight_wait(k, source, 0)
            launch(weight_over(k, source))

        ready = False
        for kind, k, left, distance, block in orders[z]:
            load(k)
            waits = kind > SUM or kind == SUM and (
                not sums[k][0] or sums[k][1] != DIRECT and seat(left) > 0
            )
            if waits and not ready:
                ready = True
                load_state()
            if kind == ACROSS:
                across(k, distance)
            elif kind == SUM:
                partial_sum(k, left, distance, block)
            elif kind == CROSS:
                cross(k)
            elif kind == UPDATE:
                update(k)
            elif kind == SPREAD:
                spread(k)
            elif kind == PASS:
                pass_on(k, left, distance, block)
            else:
                over(k, left, distance)
        for wide, out in ((ms_wide, ms_new), (vs_wide, vs_new)):
            for c in range(owned // LANES):
                span = pl.ds(c * LANES, LANES)
                out[0:1, span] = jnp.transpose(wide[span, :])[0:1, :]
        for copy in started:
            copy.wait_send()
        for k in range(pieces):
            for source in range(outer):
                for block in range(1 + spreads[k][0]):
                    if source != z:
                        weight_wait(k, source, block)
                if not spreads[k][0]:
                    weight_over(k, source).wait_recv()

    shard = lax.rem(lax.axis_index("mp"), len(turns))
    for turn in range(len(turns)):
        for z in range(outer):
            pl.when((place == z) & (shard == turn))(functools.partial(program, turn, z))


def write_out(*refs):
    sem = refs[-1]
    half = (len(refs) - 1) // 2
    copies = [
        pltpu.make_async_copy(refs[i], refs[half + i], sem.at[i]) for i in range(half)
    ]
    for copy in copies[::-1]:
        copy.start()
    for copy in copies:
        copy.wait()


def per_device(grads, master, m_codes, m_scale, v_codes, v_scale):
    outer = lax.axis_size("dp") // 2
    _, owned, width = master.shape
    plan = plan_for(outer, owned)
    sizes, turns = plan
    pieces = len(sizes)
    blocks = 1 + max(kind[0] for sums, spreads, _ in turns for kind in (*sums, *spreads))
    bf16, f32 = jnp.bfloat16, jnp.float32
    dma = pltpu.SemaphoreType.DMA
    shape = jax.ShapeDtypeStruct
    state = (1, owned, width)
    out_shapes = (
        (state, f32), (state, bf16), ((1, owned), f32),
        (state, bf16), ((1, owned), f32),
        ((1, 2 * outer * owned, width), bf16),
    )
    kept = sum(math.prod(dims) * jnp.dtype(kind).itemsize for dims, kind in out_shapes)
    outs = pl.pallas_call(
        functools.partial(kernel, outer, plan),
        out_shape=tuple(pltpu.VMEM(*each) for each in out_shapes),
        in_specs=[pl.BlockSpec(memory_space=pltpu.HBM)] * 6,
        out_specs=[pl.BlockSpec(memory_space=pltpu.VMEM)] * 6,
        scratch_shapes=[
            pltpu.VMEM((2 * outer, owned, width), bf16),
            pltpu.VMEM((outer, owned, width), bf16),
            pltpu.VMEM((outer, blocks, owned, width), bf16),
            pltpu.VMEM((outer, blocks, owned, width), bf16),
            pltpu.VMEM((outer, blocks, owned, width), bf16),
            pltpu.VMEM((owned, width), f32), pltpu.VMEM((owned, width), f32),
            pltpu.VMEM((owned, LANES), f32), pltpu.VMEM((owned, LANES), f32),
            pltpu.VMEM(state, f32), pltpu.VMEM(state, bf16), pltpu.VMEM(state, bf16),
            pltpu.VMEM((1, owned), f32), pltpu.VMEM((1, owned), f32),
            dma((pieces,)), dma((5,)),
            dma((pieces, outer)), dma((pieces, outer)),
            dma((pieces, outer, blocks)), dma((pieces, outer, blocks)), dma((pieces, outer, blocks)),
            dma((pieces, outer, blocks)), dma((pieces, outer, blocks)), dma((pieces, outer, blocks)),
            dma((pieces, outer)), dma((pieces, outer)),
        ],
        compiler_params=pltpu.CompilerParams(
            collective_id=0, has_side_effects=True,
            vmem_limit_bytes=min(VMEM_GRANT, VMEM_ALL - kept - 2**18),
        ),
    )(grads.reshape(2 * outer, owned, width), master, m_codes, m_scale, v_codes, v_scale)
    return tuple(pl.pallas_call(
        write_out,
        out_shape=tuple(shape(*each) for each in out_shapes),
        in_specs=[pl.BlockSpec(memory_space=pltpu.VMEM)] * 6,
        out_specs=[pl.BlockSpec(memory_space=pl.ANY)] * 6,
        scratch_shapes=[dma((6,))],
        compiler_params=pltpu.CompilerParams(vmem_limit_bytes=2**20),
    )(*[pltpu.with_memory_space_constraint(o, pltpu.VMEM) for o in outs]))


def solution(mesh):
    return jax.shard_map(
        per_device,
        mesh=mesh,
        in_specs=(
            P("dp", "mp", None, None),
            P("mp", "dp", None),
            P("mp", "dp", None),
            P("mp", "dp"),
            P("mp", "dp", None),
            P("mp", "dp"),
        ),
        out_specs=(
            P("mp", "dp", None),
            P("mp", "dp", None),
            P("mp", "dp"),
            P("mp", "dp", None),
            P("mp", "dp"),
            P("mp", None, None),
        ),
        check_vma=False,
    )
```

```python
import functools
import math

import jax
import jax.numpy as jnp
from jax import lax
from jax.experimental import pallas as pl
from jax.experimental.pallas import tpu as pltpu
from jax.sharding import PartitionSpec as P

STEP = 8
LANES = 128
VMEM_ALL = 67043328
VMEM_GRANT = 60 * 1024 * 1024
MESH = pl.DeviceIdType.MESH

LINE, HALF, DIRECT = 0, 1, 2
EACH, OWNER, INNER = 0, 1, 2
ACROSS, SUM, CROSS, UPDATE, SPREAD, PASS, OVER, RELAY = range(8)
CHUNK = 64
PLANS = {}


def unpacked(codes):
    return [
        (c // 100000, c // 1000 % 100, c // 100 % 10, c // 10 % 10, c % 10) for c in codes
    ]


PLANS[4] = (
    (3, 3, 3, 3, 2, 2),
    (
        (
            ((0, LINE), (0, LINE), (0, HALF), (1, LINE), (0, HALF), (0, HALF)),
            ((EACH, LINE), (EACH, LINE), (OWNER, LINE), (EACH, LINE), (EACH, LINE), (EACH, HALF)),
            (
                unpacked((
                    30, 103010, 103031, 5030, 2030, 103030, 1030, 103021, 5020, 103020, 2020, 1020, 105030,
                    103011, 5010, 2010, 101030, 4030, 105020, 100030, 1010, 4020, 101020, 4010, 105010, 102030,
                    20, 203000, 104030, 10, 101010, 5000, 104020, 2000, 104010, 1000, 100020, 303000, 4000,
                    100010, 102020, 0, 305000, 302000, 301000, 304000, 605110, 300000, 603120, 102010, 402000, 605120,
                    601110, 604110, 605130, 603130, 601120, 604120, 603110, 600120, 601130, 604130, 600130, 600110,
                )),
                unpacked((
                    30, 5030, 2030, 1030, 5000, 5020, 2000, 103021, 2020, 103020, 1000, 103011, 1020,
                    105110, 103010, 103111, 4030, 105020, 4000, 103110, 102110, 203000, 101020, 4020, 105010, 0,
                    100020, 20, 101010, 5010, 104110, 101110, 303000, 102020, 2010, 104020, 1010, 100110, 4010,
                    104010, 10, 305000, 503110, 100010, 603110, 503010, 301000, 505110, 605110, 304000, 300000, 102010,
                    503120, 505120, 605120, 501010, 501110, 504010, 604010, 603120, 604110, 504110, 500010, 502010, 500110,
                    605010, 302000, 502011, 501120, 601120, 604120, 504120, 601010, 500120, 601110, 603010, 402000, 502120,
                    600120, 502121, 600010, 502110, 600110, 502111,
                )),
                unpacked((
                    0, 5000, 2000, 1000, 5030, 5010, 2030, 103121, 2010, 103120, 1030, 103111, 1010,
                    105010, 103110, 103011, 4000, 105120, 4030, 103010, 102010, 203000, 101120, 4010, 105110, 30,
                    100120, 10, 101110, 5020, 104010, 101010, 303000, 102120, 2020, 104120, 1020, 100010, 4020,
                    104110, 20, 305000, 503010, 100110, 603010, 503110, 301000, 505010, 605010, 304000, 300000, 102110,
                    503020, 505020, 605020, 501110, 501010, 504110, 604110, 603020, 604010, 504010, 500110, 502110, 500010,
                    605110, 302000, 502111, 501020, 601020, 604020, 504020, 601110, 500020, 601010, 603110, 402000, 502020,
                    600020, 502021, 600110, 502010, 600010, 502011,
                )),
                unpacked((
                    0, 103110, 103131, 5000, 2000, 103130, 1000, 103121, 5010, 103120, 2010, 1010, 105130,
                    103111, 5020, 2020, 101130, 4000, 105120, 100130, 1020, 4010, 101120, 4020, 105110, 102130,
                    10, 203000, 104130, 20, 101110, 5030, 104120, 2030, 104110, 1030, 100120, 303000, 4030,
                    100110, 102120, 30, 305000, 302000, 301000, 304000, 605010, 300000, 603020, 102110, 402000, 605020,
                    601010, 604010, 605030, 603030, 601020, 604020, 603010, 600020, 601030, 604030, 600030, 600010,
                )),
            ),
        ),
    ),
)


def plan_for(outer, owned):
    if outer in PLANS:
        parts, turns = PLANS[outer]
        unit = owned // sum(parts)
        if unit * sum(parts) == owned and unit % 16 == 0:
            return [unit * part for part in parts], turns
    orders = []
    for z in range(outer):
        order = [(ACROSS, 0, 0, (z + 1 + step) % outer, 0) for step in range(outer)]
        for distance in range(outer - 1, 0, -1):
            order += [
                (SUM, 0, left, distance, 0) for left in (0, 1)
                if (z - distance >= 0 if left else z + distance < outer)
            ]
        order.append((UPDATE, 0, 0, 0, 0))
        for distance in range(1, outer):
            for left in (0, 1):
                if z + distance < outer if left else z - distance >= 0:
                    if z > 0 if left else z < outer - 1:
                        order.append((PASS, 0, left, distance, 0))
                    order.append((OVER, 0, left, distance, 0))
        orders.append(order)
    return [owned], [([(0, LINE)], [(EACH, LINE)], orders)]


def kernel(
    outer, plan, grads, master, m_codes, m_scale, v_codes, v_scale,
    master_new, m_new, ms_new, v_new, vs_new, weights,
    own, xgot, stage, right_got, left_got, one_kept, two_kept, ms_wide, vs_wide,
    master_in, m_in, v_in, ms_in, vs_in,
    own_sem, state_sem,
    x_send, x_recv, sum_send, right_recv, left_recv, first_send, pass_send, w_recv, a_send, a_recv,
):
    sizes, turns = plan
    pieces = len(sizes)
    starts = [sum(sizes[:k]) for k in range(pieces)]
    owned, width = master.shape[1], master.shape[2]
    replicas = 2 * outer
    f32, bf16 = jnp.float32, jnp.bfloat16
    me = lax.axis_index("dp")
    x = lax.rem(me, 2)
    place = lax.div(me, 2)
    other = place * 2 + 1 - x

    forms = [form for sums, spreads, _ in turns for _, form in (*sums, *spreads)]
    reach = outer - 1 if DIRECT in forms else max(1, outer - 2) if HALF in forms else 1
    barrier = pltpu.get_barrier_semaphore()
    pl.semaphore_signal(barrier, inc=1, device_id={"dp": other}, device_id_type=MESH)
    for step in range(1, reach + 1):
        for near, inside in ((place - step, place >= step), (place + step, place + step < outer)):
            pl.when(inside)(functools.partial(
                pl.semaphore_signal, barrier, inc=1, device_id={"dp": near * 2 + x}, device_id_type=MESH
            ))

    def rows_in(k):
        return pl.ds(starts[k], sizes[k])

    own_copies = [
        pltpu.make_async_copy(grads.at[:, rows_in(k), :], own.at[:, rows_in(k), :], own_sem.at[k])
        for k in range(pieces)
    ]
    state_copies = [
        pltpu.make_async_copy(src, dst, state_sem.at[i])
        for i, (src, dst) in enumerate((
            (master, master_in), (m_codes, m_in), (v_codes, v_in), (m_scale, ms_in), (v_scale, vs_in),
        ))
    ]
    uses = list(dict.fromkeys(step[1] for step in turns[0][2][0]))
    for k in uses:
        own_copies[k].start()
    for copy in state_copies:
        copy.start()
    near = sum(
        (place >= step).astype(jnp.int32) + (place + step < outer).astype(jnp.int32)
        for step in range(1, reach + 1)
    )
    pl.semaphore_wait(barrier, 1 + near)

    def remote(src, dst, send, recv, device):
        return pltpu.make_async_remote_copy(
            src_ref=src, dst_ref=dst, send_sem=send, recv_sem=recv,
            device_id={"dp": device}, device_id_type=MESH,
        )

    def column(block):
        return 1 - x if block else x

    def in_rows(k, body):
        chunk = min(CHUNK, sizes[k])
        count = sizes[k] // chunk
        if count <= 2 and count * chunk == sizes[k]:
            for c in range(count):
                body(pl.ds(starts[k] + c * chunk, chunk))
        elif count * chunk == sizes[k]:
            lax.fori_loop(
                0, count, lambda c, _: body(pl.ds(pl.multiple_of(starts[k] + c * chunk, 16), chunk)), None
            )
        else:
            body(rows_in(k))

    def program(turn, z):
        sums, spreads, orders = turns[turn]
        started = []
        taken = set()
        loaded = set()

        def load(k):
            if k not in loaded:
                loaded.add(k)
                own_copies[k].wait()

        def load_state():
            for copy in state_copies:
                copy.wait()
            for source, wide in ((ms_in, ms_wide), (vs_in, vs_wide)):
                for c in range(owned // LANES):
                    span = pl.ds(c * LANES, LANES)
                    wide[span, :] = jnp.transpose(jnp.broadcast_to(source[0:1, span], (LANES, LANES)))

        def launch(copy):
            copy.start()
            started.append(copy)

        def seat(left):
            return outer - 1 - z if left else z

        def at(left, number):
            return outer - 1 - number if left else number

        def x_copy(k, t, src):
            return remote(src, xgot.at[t, rows_in(k), :], x_send.at[k, t], x_recv.at[k, t], other)

        def x_wait(k, t):
            x_copy(k, t, xgot.at[t, rows_in(k), :]).wait_recv()

        def across(k, t):
            launch(x_copy(k, t, own.at[t * 2 + 1 - x, rows_in(k), :]))

        def got_of(left):
            return (left_got, left_recv) if left else (right_got, right_recv)

        def sum_wait(k, left, slot, block):
            got, recv = got_of(left)
            ref = got.at[slot, block, rows_in(k), :]
            remote(ref, ref, sum_send.at[k, slot, block], recv.at[k, slot, block], other).wait_recv()

        def add_up(k, t, block, terms, rows):
            total = own[t * 2 + column(block), rows, :].astype(f32)
            if not sums[k][0]:
                total = total + xgot[t, rows, :].astype(f32)
            for left, slot in terms:
                total = total + got_of(left)[0][slot, block, rows, :].astype(f32)
            return total

        def partial_sum(k, left, distance, block):
            z_first, form = sums[k]
            got, recv = got_of(left)
            seated = seat(left)
            t = at(left, seated + distance)
            adds = form == LINE and seated > 0 or form == HALF and seated == 1
            hops = form == LINE or form == HALF and seated == 0
            slot = t if hops else z
            dest = at(left, seated + 1) if hops else t
            if z_first and not adds:
                src = own.at[t * 2 + column(block), rows_in(k), :]
            else:
                if not z_first:
                    x_wait(k, t)
                if adds:
                    sum_wait(k, left, t, block)

                def body(rows):
                    if adds and z_first:
                        total = own[t * 2 + column(block), rows, :] + got[t, block, rows, :]
                    elif adds:
                        total = add_up(k, t, block, [(left, t)], rows)
                    else:
                        total = own[t * 2 + column(block), rows, :] + xgot[t, rows, :]
                    stage[t, block, rows, :] = total.astype(bf16)
                in_rows(k, body)
                src = stage.at[t, block, rows_in(k), :]
            launch(remote(
                src, got.at[slot, block, rows_in(k), :], sum_send.at[k, t, block],
                recv.at[k, slot, block], dest * 2 + x,
            ))

        def arrived(k, block):
            form = sums[k][1]
            terms = []
            for left in (0, 1):
                seated = seat(left)
                if seated == 0:
                    continue
                if form == LINE or form == HALF and seated == 1:
                    terms.append((left, z))
                else:
                    terms += [(left, at(left, s)) for s in range(1 if form == HALF else 0, seated)]
            if not sums[k][0]:
                x_wait(k, z)
            for left, slot in terms:
                sum_wait(k, left, slot, block)
            return terms

        def cross(k):
            terms = arrived(k, 1)

            def body(rows):
                stage[z, 1, rows, :] = add_up(k, z, 1, terms, rows).astype(bf16)
            in_rows(k, body)
            launch(x_copy(k, z, stage.at[z, 1, rows_in(k), :]))

        def weight_rows(k, source, block):
            start = (source * 2 + column(block)) * owned + starts[k]
            return weights.at[0, pl.ds(pl.multiple_of(start, 16), sizes[k]), :]

        def weight_copy(k, source, block, send, dest):
            rows = weight_rows(k, source, block)
            return remote(rows, rows, send, w_recv.at[k, source, block], dest * 2 + x)

        def weight_wait(k, source, block):
            if (k, source, block) not in taken:
                taken.add((k, source, block))
                weight_copy(k, source, block, pass_send.at[k, source, block], z).wait_recv()

        def weight_over(k, source):
            rows = weight_rows(k, source, 0)
            return remote(rows, rows, a_send.at[k, source], a_recv.at[k, source], other)

        def first_sends(k, block):
            form = spreads[k][1]
            for left in (0, 1):
                seated = seat(left)
                last = outer - 1
                if seated == last:
                    continue
                if form == LINE or form == HALF and seated == last - 1:
                    dests = [seated + 1]
                else:
                    dests = range(last if form == DIRECT else last - 1, seated, -1)
                for number in dests:
                    dest = at(left, number)
                    launch(weight_copy(k, z, block, first_send.at[k, dest, block], dest))

        def update(k):
            terms = arrived(k, 0)
            if sums[k][0]:
                x_wait(k, z)
            repeat = width // LANES
            first_fix = 1.0 - 0.9**STEP
            second_fix = 1.0 - 0.95**STEP

            def body(rows):
                value = add_up(k, z, 0, terms, rows)
                if sums[k][0]:
                    value = value + xgot[z, rows, :].astype(f32)
                mean = value * (1.0 / replicas)
                ms = jnp.concatenate([ms_wide[rows, :]] * repeat, axis=1)
                vs = jnp.concatenate([vs_wide[rows, :]] * repeat, axis=1)
                one = 0.9 * m_in[0, rows].astype(f32) * ms + 0.1 * mean
                two = 0.95 * v_in[0, rows].astype(f32) * vs + 0.05 * mean * mean
                new = master_in[0, rows] - (0.1 / first_fix) * one / (
                    jnp.sqrt(two * (1.0 / second_fix)) + 1e-08
                )
                mine = pl.ds(pl.multiple_of(me * owned + rows.start, 16), rows.size)
                weights[0, mine, :] = new.astype(bf16)
                master_new[0, rows] = new
                one_kept[rows, :] = one
                two_kept[rows, :] = two

            def code(rows):
                one = one_kept[rows, :]
                two = two_kept[rows, :]
                one_top = jnp.max(jnp.abs(one), axis=-1, keepdims=True) + 1e-06
                two_top = jnp.max(jnp.abs(two), axis=-1, keepdims=True) + 1e-06
                m_new[0, rows] = (one / one_top).astype(bf16)
                v_new[0, rows] = (two / two_top).astype(bf16)
                ms_wide[rows, :] = jnp.broadcast_to(one_top, (rows.size, LANES))
                vs_wide[rows, :] = jnp.broadcast_to(two_top, (rows.size, LANES))
            in_rows(k, body)
            if spreads[k][0] == OWNER:
                launch(weight_over(k, z))
            first_sends(k, 0)
            if spreads[k][0] != OWNER:
                launch(weight_over(k, z))
            in_rows(k, code)

        def spread(k):
            weight_over(k, z).wait_recv()
            first_sends(k, 1)

        def pass_on(k, left, apart, block):
            source = at(left, seat(left) - apart)
            weight_wait(k, source, block)
            launch(weight_copy(
                k, source, block, pass_send.at[k, source, block], at(left, seat(left) + 1)
            ))

        def over(k, left, apart):
            source = at(left, seat(left) - apart)
            weight_wait(k, source, 0)
            launch(weight_over(k, source))

        def over_wait(k, source):
            if (k, source) not in taken:
                taken.add((k, source))
                weight_over(k, source).wait_recv()

        def relay(k, left, source):
            over_wait(k, source)
            launch(weight_copy(
                k, source, 1, pass_send.at[k, source, 1], at(left, seat(left) + 1)
            ))

        ready = False
        for kind, k, left, distance, block in orders[z]:
            load(k)
            waits = kind > SUM or kind == SUM and (
                not sums[k][0] or sums[k][1] != DIRECT and seat(left) > 0
            )
            if waits and not ready:
                ready = True
                load_state()
            if kind == ACROSS:
                across(k, distance)
            elif kind == SUM:
                partial_sum(k, left, distance, block)
            elif kind == CROSS:
                cross(k)
            elif kind == UPDATE:
                update(k)
            elif kind == SPREAD:
                spread(k)
            elif kind == PASS:
                pass_on(k, left, distance, block)
            elif kind == OVER:
                over(k, left, distance)
            else:
                relay(k, left, distance)
        for wide, out in ((ms_wide, ms_new), (vs_wide, vs_new)):
            for c in range(owned // LANES):
                span = pl.ds(c * LANES, LANES)
                out[0:1, span] = jnp.transpose(wide[span, :])[0:1, :]
        for copy in started:
            copy.wait_send()
        for k in range(pieces):
            crossing = spreads[k][0]
            ends = crossing == INNER and z in (0, outer - 1)
            for source in range(outer):
                if source != z:
                    weight_wait(k, source, 0)
                    if crossing == OWNER or ends:
                        weight_wait(k, source, 1)
                if crossing != OWNER and (source == z or not ends):
                    over_wait(k, source)

    shard = lax.rem(lax.axis_index("mp"), len(turns))
    for turn in range(len(turns)):
        for z in range(outer):
            pl.when((place == z) & (shard == turn))(functools.partial(program, turn, z))


def write_out(*refs):
    sem = refs[-1]
    half = (len(refs) - 1) // 2
    copies = [
        pltpu.make_async_copy(refs[i], refs[half + i], sem.at[i]) for i in range(half)
    ]
    for copy in copies[::-1]:
        copy.start()
    for copy in copies:
        copy.wait()


def per_device(grads, master, m_codes, m_scale, v_codes, v_scale):
    outer = lax.axis_size("dp") // 2
    _, owned, width = master.shape
    plan = plan_for(outer, owned)
    sizes, turns = plan
    pieces = len(sizes)
    blocks = 1 + max(min(kind[0], 1) for sums, spreads, _ in turns for kind in (*sums, *spreads))
    bf16, f32 = jnp.bfloat16, jnp.float32
    dma = pltpu.SemaphoreType.DMA
    shape = jax.ShapeDtypeStruct
    state = (1, owned, width)
    out_shapes = (
        (state, f32), (state, bf16), ((1, owned), f32),
        (state, bf16), ((1, owned), f32),
        ((1, 2 * outer * owned, width), bf16),
    )
    kept = sum(math.prod(dims) * jnp.dtype(kind).itemsize for dims, kind in out_shapes)
    outs = pl.pallas_call(
        functools.partial(kernel, outer, plan),
        out_shape=tuple(pltpu.VMEM(*each) for each in out_shapes),
        in_specs=[pl.BlockSpec(memory_space=pltpu.HBM)] * 6,
        out_specs=[pl.BlockSpec(memory_space=pltpu.VMEM)] * 6,
        scratch_shapes=[
            pltpu.VMEM((2 * outer, owned, width), bf16),
            pltpu.VMEM((outer, owned, width), bf16),
            pltpu.VMEM((outer, blocks, owned, width), bf16),
            pltpu.VMEM((outer, blocks, owned, width), bf16),
            pltpu.VMEM((outer, blocks, owned, width), bf16),
            pltpu.VMEM((owned, width), f32), pltpu.VMEM((owned, width), f32),
            pltpu.VMEM((owned, LANES), f32), pltpu.VMEM((owned, LANES), f32),
            pltpu.VMEM(state, f32), pltpu.VMEM(state, bf16), pltpu.VMEM(state, bf16),
            pltpu.VMEM((1, owned), f32), pltpu.VMEM((1, owned), f32),
            dma((pieces,)), dma((5,)),
            dma((pieces, outer)), dma((pieces, outer)),
            dma((pieces, outer, blocks)), dma((pieces, outer, blocks)), dma((pieces, outer, blocks)),
            dma((pieces, outer, blocks)), dma((pieces, outer, blocks)), dma((pieces, outer, blocks)),
            dma((pieces, outer)), dma((pieces, outer)),
        ],
        compiler_params=pltpu.CompilerParams(
            collective_id=0, has_side_effects=True,
            vmem_limit_bytes=min(VMEM_GRANT, VMEM_ALL - kept - 2**18),
        ),
    )(grads.reshape(2 * outer, owned, width), master, m_codes, m_scale, v_codes, v_scale)
    return tuple(pl.pallas_call(
        write_out,
        out_shape=tuple(shape(*each) for each in out_shapes),
        in_specs=[pl.BlockSpec(memory_space=pltpu.VMEM)] * 6,
        out_specs=[pl.BlockSpec(memory_space=pl.ANY)] * 6,
        scratch_shapes=[dma((6,))],
        compiler_params=pltpu.CompilerParams(vmem_limit_bytes=2**20),
    )(*[pltpu.with_memory_space_constraint(o, pltpu.VMEM) for o in outs]))


def solution(mesh):
    return jax.shard_map(
        per_device,
        mesh=mesh,
        in_specs=(
            P("dp", "mp", None, None),
            P("mp", "dp", None),
            P("mp", "dp", None),
            P("mp", "dp"),
            P("mp", "dp", None),
            P("mp", "dp"),
        ),
        out_specs=(
            P("mp", "dp", None),
            P("mp", "dp", None),
            P("mp", "dp"),
            P("mp", "dp", None),
            P("mp", "dp"),
            P("mp", None, None),
        ),
        check_vma=False,
    )
```

```python
import functools
import math

import jax
import jax.numpy as jnp
from jax import lax
from jax.experimental import pallas as pl
from jax.experimental.pallas import tpu as pltpu
from jax.sharding import PartitionSpec as P

STEP = 8
LANES = 128
VMEM_ALL = 67043328
VMEM_GRANT = 60 * 1024 * 1024
MESH = pl.DeviceIdType.MESH

LINE, HALF, DIRECT = 0, 1, 2
EACH, OWNER, INNER = 0, 1, 2
ACROSS, SUM, CROSS, UPDATE, SPREAD, PASS, OVER, RELAY = range(8)
CHUNK = 48
PLANS = {}


def unpacked(codes):
    return [
        (c // 100000, c // 1000 % 100, c // 100 % 10, c // 10 % 10, c % 10) for c in codes
    ]


PLANS[4] = (
    (3, 3, 3, 3, 2, 2),
    (
        (
            ((0, LINE), (0, LINE), (0, HALF), (1, LINE), (0, HALF), (0, HALF)),
            ((EACH, LINE), (EACH, LINE), (OWNER, LINE), (EACH, LINE), (EACH, LINE), (EACH, HALF)),
            (
                unpacked((
                    30, 103010, 103031, 5030, 2030, 103030, 1030, 103021, 5020, 103020, 2020, 1020, 105030,
                    103011, 5010, 2010, 101030, 4030, 105020, 100030, 1010, 4020, 101020, 4010, 105010, 102030,
                    20, 203000, 104030, 10, 101010, 5000, 104020, 2000, 104010, 1000, 100020, 303000, 4000,
                    100010, 102020, 0, 305000, 302000, 301000, 304000, 605110, 300000, 603120, 102010, 402000, 605120,
                    601110, 604110, 605130, 603130, 601120, 604120, 603110, 600120, 601130, 604130, 600130, 600110,
                )),
                unpacked((
                    30, 5030, 2030, 1030, 5000, 5020, 2000, 103021, 2020, 103020, 1000, 103011, 1020,
                    105110, 103010, 103111, 4030, 105020, 4000, 103110, 102110, 203000, 101020, 4020, 105010, 0,
                    100020, 20, 101010, 5010, 104110, 101110, 303000, 102020, 2010, 104020, 1010, 100110, 4010,
                    104010, 10, 305000, 503110, 100010, 603110, 503010, 301000, 505110, 605110, 304000, 300000, 102010,
                    503120, 505120, 605120, 501010, 501110, 504010, 604010, 603120, 604110, 504110, 500010, 502010, 500110,
                    605010, 302000, 502011, 501120, 601120, 604120, 504120, 601010, 500120, 601110, 603010, 402000, 502120,
                    600120, 502121, 600010, 502110, 600110, 502111,
                )),
                unpacked((
                    0, 5000, 2000, 1000, 5030, 5010, 2030, 103121, 2010, 103120, 1030, 103111, 1010,
                    105010, 103110, 103011, 4000, 105120, 4030, 103010, 102010, 203000, 101120, 4010, 105110, 30,
                    100120, 10, 101110, 5020, 104010, 101010, 303000, 102120, 2020, 104120, 1020, 100010, 4020,
                    104110, 20, 305000, 503010, 100110, 603010, 503110, 301000, 505010, 605010, 304000, 300000, 102110,
                    503020, 505020, 605020, 501110, 501010, 504110, 604110, 603020, 604010, 504010, 500110, 502110, 500010,
                    605110, 302000, 502111, 501020, 601020, 604020, 504020, 601110, 500020, 601010, 603110, 402000, 502020,
                    600020, 502021, 600110, 502010, 600010, 502011,
                )),
                unpacked((
                    0, 103110, 103131, 5000, 2000, 103130, 1000, 103121, 5010, 103120, 2010, 1010, 105130,
                    103111, 5020, 2020, 101130, 4000, 105120, 100130, 1020, 4010, 101120, 4020, 105110, 102130,
                    10, 203000, 104130, 20, 101110, 5030, 104120, 2030, 104110, 1030, 100120, 303000, 4030,
                    100110, 102120, 30, 305000, 302000, 301000, 304000, 605010, 300000, 603020, 102110, 402000, 605020,
                    601010, 604010, 605030, 603030, 601020, 604020, 603010, 600020, 601030, 604030, 600030, 600010,
                )),
            ),
        ),
    ),
)


def plan_for(outer, owned):
    if outer in PLANS:
        parts, turns = PLANS[outer]
        unit = owned // sum(parts)
        if unit * sum(parts) == owned and unit % 16 == 0:
            return [unit * part for part in parts], turns
    orders = []
    for z in range(outer):
        order = [(ACROSS, 0, 0, (z + 1 + step) % outer, 0) for step in range(outer)]
        for distance in range(outer - 1, 0, -1):
            order += [
                (SUM, 0, left, distance, 0) for left in (0, 1)
                if (z - distance >= 0 if left else z + distance < outer)
            ]
        order.append((UPDATE, 0, 0, 0, 0))
        for distance in range(1, outer):
            for left in (0, 1):
                if z + distance < outer if left else z - distance >= 0:
                    if z > 0 if left else z < outer - 1:
                        order.append((PASS, 0, left, distance, 0))
                    order.append((OVER, 0, left, distance, 0))
        orders.append(order)
    return [owned], [([(0, LINE)], [(EACH, LINE)], orders)]


def kernel(
    outer, plan, grads, master, m_codes, m_scale, v_codes, v_scale,
    master_new, m_new, ms_new, v_new, vs_new, weights,
    own, xgot, stage, right_got, left_got, one_kept, two_kept, ms_wide, vs_wide,
    master_in, m_in, v_in, ms_in, vs_in,
    own_sem, state_sem,
    x_send, x_recv, sum_send, right_recv, left_recv, first_send, pass_send, w_recv, a_send, a_recv,
):
    sizes, turns = plan
    pieces = len(sizes)
    starts = [sum(sizes[:k]) for k in range(pieces)]
    owned, width = master.shape[1], master.shape[2]
    replicas = 2 * outer
    f32, bf16 = jnp.float32, jnp.bfloat16
    me = lax.axis_index("dp")
    x = lax.rem(me, 2)
    place = lax.div(me, 2)
    other = place * 2 + 1 - x

    forms = [form for sums, spreads, _ in turns for _, form in (*sums, *spreads)]
    reach = outer - 1 if DIRECT in forms else max(1, outer - 2) if HALF in forms else 1
    barrier = pltpu.get_barrier_semaphore()
    pl.semaphore_signal(barrier, inc=1, device_id={"dp": other}, device_id_type=MESH)
    for step in range(1, reach + 1):
        for near, inside in ((place - step, place >= step), (place + step, place + step < outer)):
            pl.when(inside)(functools.partial(
                pl.semaphore_signal, barrier, inc=1, device_id={"dp": near * 2 + x}, device_id_type=MESH
            ))

    def rows_in(k):
        return pl.ds(starts[k], sizes[k])

    own_copies = [
        pltpu.make_async_copy(grads.at[:, rows_in(k), :], own.at[:, rows_in(k), :], own_sem.at[k])
        for k in range(pieces)
    ]
    state_copies = [
        pltpu.make_async_copy(src, dst, state_sem.at[i])
        for i, (src, dst) in enumerate((
            (master, master_in), (m_codes, m_in), (v_codes, v_in), (m_scale, ms_in), (v_scale, vs_in),
        ))
    ]
    uses = list(dict.fromkeys(step[1] for step in turns[0][2][0]))
    for k in uses:
        own_copies[k].start()
    for copy in state_copies:
        copy.start()
    near = sum(
        (place >= step).astype(jnp.int32) + (place + step < outer).astype(jnp.int32)
        for step in range(1, reach + 1)
    )
    pl.semaphore_wait(barrier, 1 + near)

    def remote(src, dst, send, recv, device):
        return pltpu.make_async_remote_copy(
            src_ref=src, dst_ref=dst, send_sem=send, recv_sem=recv,
            device_id={"dp": device}, device_id_type=MESH,
        )

    def column(block):
        return 1 - x if block else x

    def in_rows(k, body):
        chunk = min(CHUNK, sizes[k])
        count = sizes[k] // chunk
        if count <= 2 and count * chunk == sizes[k]:
            for c in range(count):
                body(pl.ds(starts[k] + c * chunk, chunk))
        elif count * chunk == sizes[k]:
            lax.fori_loop(
                0, count, lambda c, _: body(pl.ds(pl.multiple_of(starts[k] + c * chunk, 16), chunk)), None
            )
        else:
            body(rows_in(k))

    def program(turn, z):
        sums, spreads, orders = turns[turn]
        started = []
        taken = set()
        loaded = set()

        def load(k):
            if k not in loaded:
                loaded.add(k)
                own_copies[k].wait()

        def load_state():
            for copy in state_copies:
                copy.wait()
            for source, wide in ((ms_in, ms_wide), (vs_in, vs_wide)):
                for c in range(owned // LANES):
                    span = pl.ds(c * LANES, LANES)
                    wide[span, :] = jnp.transpose(jnp.broadcast_to(source[0:1, span], (LANES, LANES)))

        def launch(copy):
            copy.start()
            started.append(copy)

        def seat(left):
            return outer - 1 - z if left else z

        def at(left, number):
            return outer - 1 - number if left else number

        def x_copy(k, t, src):
            return remote(src, xgot.at[t, rows_in(k), :], x_send.at[k, t], x_recv.at[k, t], other)

        def x_wait(k, t):
            x_copy(k, t, xgot.at[t, rows_in(k), :]).wait_recv()

        def across(k, t):
            launch(x_copy(k, t, own.at[t * 2 + 1 - x, rows_in(k), :]))

        def got_of(left):
            return (left_got, left_recv) if left else (right_got, right_recv)

        def sum_wait(k, left, slot, block):
            got, recv = got_of(left)
            ref = got.at[slot, block, rows_in(k), :]
            remote(ref, ref, sum_send.at[k, slot, block], recv.at[k, slot, block], other).wait_recv()

        def add_up(k, t, block, terms, rows):
            total = own[t * 2 + column(block), rows, :].astype(f32)
            if not sums[k][0]:
                total = total + xgot[t, rows, :].astype(f32)
            for left, slot in terms:
                total = total + got_of(left)[0][slot, block, rows, :].astype(f32)
            return total

        def partial_sum(k, left, distance, block):
            z_first, form = sums[k]
            got, recv = got_of(left)
            seated = seat(left)
            t = at(left, seated + distance)
            adds = form == LINE and seated > 0 or form == HALF and seated == 1
            hops = form == LINE or form == HALF and seated == 0
            slot = t if hops else z
            dest = at(left, seated + 1) if hops else t
            if z_first and not adds:
                src = own.at[t * 2 + column(block), rows_in(k), :]
            else:
                if not z_first:
                    x_wait(k, t)
                if adds:
                    sum_wait(k, left, t, block)

                def body(rows):
                    if adds and z_first:
                        total = own[t * 2 + column(block), rows, :] + got[t, block, rows, :]
                    elif adds:
                        total = add_up(k, t, block, [(left, t)], rows)
                    else:
                        total = own[t * 2 + column(block), rows, :] + xgot[t, rows, :]
                    stage[t, block, rows, :] = total.astype(bf16)
                in_rows(k, body)
                src = stage.at[t, block, rows_in(k), :]
            launch(remote(
                src, got.at[slot, block, rows_in(k), :], sum_send.at[k, t, block],
                recv.at[k, slot, block], dest * 2 + x,
            ))

        def arrived(k, block):
            form = sums[k][1]
            terms = []
            for left in (0, 1):
                seated = seat(left)
                if seated == 0:
                    continue
                if form == LINE or form == HALF and seated == 1:
                    terms.append((left, z))
                else:
                    terms += [(left, at(left, s)) for s in range(1 if form == HALF else 0, seated)]
            if not sums[k][0]:
                x_wait(k, z)
            for left, slot in terms:
                sum_wait(k, left, slot, block)
            return terms

        def cross(k):
            terms = arrived(k, 1)

            def body(rows):
                stage[z, 1, rows, :] = add_up(k, z, 1, terms, rows).astype(bf16)
            in_rows(k, body)
            launch(x_copy(k, z, stage.at[z, 1, rows_in(k), :]))

        def weight_rows(k, source, block):
            start = (source * 2 + column(block)) * owned + starts[k]
            return weights.at[0, pl.ds(pl.multiple_of(start, 16), sizes[k]), :]

        def weight_copy(k, source, block, send, dest):
            rows = weight_rows(k, source, block)
            return remote(rows, rows, send, w_recv.at[k, source, block], dest * 2 + x)

        def weight_wait(k, source, block):
            if (k, source, block) not in taken:
                taken.add((k, source, block))
                weight_copy(k, source, block, pass_send.at[k, source, block], z).wait_recv()

        def weight_over(k, source):
            rows = weight_rows(k, source, 0)
            return remote(rows, rows, a_send.at[k, source], a_recv.at[k, source], other)

        def first_sends(k, block):
            form = spreads[k][1]
            for left in (0, 1):
                seated = seat(left)
                last = outer - 1
                if seated == last:
                    continue
                if form == LINE or form == HALF and seated == last - 1:
                    dests = [seated + 1]
                else:
                    dests = range(last if form == DIRECT else last - 1, seated, -1)
                for number in dests:
                    dest = at(left, number)
                    launch(weight_copy(k, z, block, first_send.at[k, dest, block], dest))

        def update(k):
            terms = arrived(k, 0)
            if sums[k][0]:
                x_wait(k, z)
            repeat = width // LANES
            first_fix = 1.0 - 0.9**STEP
            second_fix = 1.0 - 0.95**STEP

            def body(rows):
                value = add_up(k, z, 0, terms, rows)
                if sums[k][0]:
                    value = value + xgot[z, rows, :].astype(f32)
                mean = value * (1.0 / replicas)
                ms = jnp.concatenate([ms_wide[rows, :]] * repeat, axis=1)
                vs = jnp.concatenate([vs_wide[rows, :]] * repeat, axis=1)
                one = 0.9 * m_in[0, rows].astype(f32) * ms + 0.1 * mean
                two = 0.95 * v_in[0, rows].astype(f32) * vs + 0.05 * mean * mean
                new = master_in[0, rows] - (0.1 / first_fix) * one / (
                    jnp.sqrt(two * (1.0 / second_fix)) + 1e-08
                )
                mine = pl.ds(pl.multiple_of(me * owned + rows.start, 16), rows.size)
                weights[0, mine, :] = new.astype(bf16)
                master_new[0, rows] = new
                one_kept[rows, :] = one
                two_kept[rows, :] = two

            def code(rows):
                one = one_kept[rows, :]
                two = two_kept[rows, :]
                one_top = jnp.max(jnp.abs(one), axis=-1, keepdims=True) + 1e-06
                two_top = jnp.max(jnp.abs(two), axis=-1, keepdims=True) + 1e-06
                m_new[0, rows] = (one / one_top).astype(bf16)
                v_new[0, rows] = (two / two_top).astype(bf16)
                ms_wide[rows, :] = jnp.broadcast_to(one_top, (rows.size, LANES))
                vs_wide[rows, :] = jnp.broadcast_to(two_top, (rows.size, LANES))
            in_rows(k, body)
            if spreads[k][0] == OWNER:
                launch(weight_over(k, z))
            first_sends(k, 0)
            if spreads[k][0] != OWNER:
                launch(weight_over(k, z))
            in_rows(k, code)

        def spread(k):
            weight_over(k, z).wait_recv()
            first_sends(k, 1)

        def pass_on(k, left, apart, block):
            source = at(left, seat(left) - apart)
            weight_wait(k, source, block)
            launch(weight_copy(
                k, source, block, pass_send.at[k, source, block], at(left, seat(left) + 1)
            ))

        def over(k, left, apart):
            source = at(left, seat(left) - apart)
            weight_wait(k, source, 0)
            launch(weight_over(k, source))

        def over_wait(k, source):
            if (k, source) not in taken:
                taken.add((k, source))
                weight_over(k, source).wait_recv()

        def relay(k, left, source):
            over_wait(k, source)
            launch(weight_copy(
                k, source, 1, pass_send.at[k, source, 1], at(left, seat(left) + 1)
            ))

        ready = False
        for kind, k, left, distance, block in orders[z]:
            load(k)
            waits = kind > SUM or kind == SUM and (
                not sums[k][0] or sums[k][1] != DIRECT and seat(left) > 0
            )
            if waits and not ready:
                ready = True
                load_state()
            if kind == ACROSS:
                across(k, distance)
            elif kind == SUM:
                partial_sum(k, left, distance, block)
            elif kind == CROSS:
                cross(k)
            elif kind == UPDATE:
                update(k)
            elif kind == SPREAD:
                spread(k)
            elif kind == PASS:
                pass_on(k, left, distance, block)
            elif kind == OVER:
                over(k, left, distance)
            else:
                relay(k, left, distance)
        for wide, out in ((ms_wide, ms_new), (vs_wide, vs_new)):
            for c in range(owned // LANES):
                span = pl.ds(c * LANES, LANES)
                out[0:1, span] = jnp.transpose(wide[span, :])[0:1, :]
        for copy in started:
            copy.wait_send()
        for k in range(pieces):
            crossing = spreads[k][0]
            ends = crossing == INNER and z in (0, outer - 1)
            for source in range(outer):
                if source != z:
                    weight_wait(k, source, 0)
                    if crossing == OWNER or ends:
                        weight_wait(k, source, 1)
                if crossing != OWNER and (source == z or not ends):
                    over_wait(k, source)

    shard = lax.rem(lax.axis_index("mp"), len(turns))
    for turn in range(len(turns)):
        for z in range(outer):
            pl.when((place == z) & (shard == turn))(functools.partial(program, turn, z))


def write_out(*refs):
    sem = refs[-1]
    half = (len(refs) - 1) // 2
    copies = [
        pltpu.make_async_copy(refs[i], refs[half + i], sem.at[i]) for i in range(half)
    ]
    for copy in copies[::-1]:
        copy.start()
    for copy in copies:
        copy.wait()


def per_device(grads, master, m_codes, m_scale, v_codes, v_scale):
    outer = lax.axis_size("dp") // 2
    _, owned, width = master.shape
    plan = plan_for(outer, owned)
    sizes, turns = plan
    pieces = len(sizes)
    blocks = 1 + max(min(kind[0], 1) for sums, spreads, _ in turns for kind in (*sums, *spreads))
    bf16, f32 = jnp.bfloat16, jnp.float32
    dma = pltpu.SemaphoreType.DMA
    shape = jax.ShapeDtypeStruct
    state = (1, owned, width)
    out_shapes = (
        (state, f32), (state, bf16), ((1, owned), f32),
        (state, bf16), ((1, owned), f32),
        ((1, 2 * outer * owned, width), bf16),
    )
    kept = sum(math.prod(dims) * jnp.dtype(kind).itemsize for dims, kind in out_shapes)
    outs = pl.pallas_call(
        functools.partial(kernel, outer, plan),
        out_shape=tuple(pltpu.VMEM(*each) for each in out_shapes),
        in_specs=[pl.BlockSpec(memory_space=pltpu.HBM)] * 6,
        out_specs=[pl.BlockSpec(memory_space=pltpu.VMEM)] * 6,
        scratch_shapes=[
            pltpu.VMEM((2 * outer, owned, width), bf16),
            pltpu.VMEM((outer, owned, width), bf16),
            pltpu.VMEM((outer, blocks, owned, width), bf16),
            pltpu.VMEM((outer, blocks, owned, width), bf16),
            pltpu.VMEM((outer, blocks, owned, width), bf16),
            pltpu.VMEM((owned, width), f32), pltpu.VMEM((owned, width), f32),
            pltpu.VMEM((owned, LANES), f32), pltpu.VMEM((owned, LANES), f32),
            pltpu.VMEM(state, f32), pltpu.VMEM(state, bf16), pltpu.VMEM(state, bf16),
            pltpu.VMEM((1, owned), f32), pltpu.VMEM((1, owned), f32),
            dma((pieces,)), dma((5,)),
            dma((pieces, outer)), dma((pieces, outer)),
            dma((pieces, outer, blocks)), dma((pieces, outer, blocks)), dma((pieces, outer, blocks)),
            dma((pieces, outer, blocks)), dma((pieces, outer, blocks)), dma((pieces, outer, blocks)),
            dma((pieces, outer)), dma((pieces, outer)),
        ],
        compiler_params=pltpu.CompilerParams(
            collective_id=0, has_side_effects=True,
            vmem_limit_bytes=min(VMEM_GRANT, VMEM_ALL - kept - 2**18),
        ),
    )(grads.reshape(2 * outer, owned, width), master, m_codes, m_scale, v_codes, v_scale)
    return tuple(pl.pallas_call(
        write_out,
        out_shape=tuple(shape(*each) for each in out_shapes),
        in_specs=[pl.BlockSpec(memory_space=pltpu.VMEM)] * 6,
        out_specs=[pl.BlockSpec(memory_space=pl.ANY)] * 6,
        scratch_shapes=[dma((6,))],
        compiler_params=pltpu.CompilerParams(vmem_limit_bytes=2**20),
    )(*[pltpu.with_memory_space_constraint(o, pltpu.VMEM) for o in outs]))


def solution(mesh):
    return jax.shard_map(
        per_device,
        mesh=mesh,
        in_specs=(
            P("dp", "mp", None, None),
            P("mp", "dp", None),
            P("mp", "dp", None),
            P("mp", "dp"),
            P("mp", "dp", None),
            P("mp", "dp"),
        ),
        out_specs=(
            P("mp", "dp", None),
            P("mp", "dp", None),
            P("mp", "dp"),
            P("mp", "dp", None),
            P("mp", "dp"),
            P("mp", None, None),
        ),
        check_vma=False,
    )
```
